32 devices in a mesh: prow: 4 (over y, core), pcol: 8 (over z, x).
Axes of the slice: x: 2, y: 2, z: 4, core: 2. Of those that a mesh axis runs over, the one named last changes fastest.
Arguments:
- slab: bfloat16 [8192, 3072], P('prow', 'pcol'), may hold values from -6 to 6
- pivots: int32 [512], replicated, may hold values from 0 to 8191, as said below
- l_top: bfloat16 [512, 512], replicated, may hold values from -0.125 to 0.125
- l_panel_t: bfloat16 [512, 8192], P('pcol', 'prow'), may hold values from -0.125 to 0.125
Outputs:
- result: bfloat16 [8192, 3072], P('prow', 'pcol')
The draws below stay inside these ranges and needn't reach their ends.
Inputs may be any that keep to these rules, and one draw needn't show every extreme that they name: `pivots`: distinct rows; how many fall on each index of prow is uneven and changes with the draw.
All inputs are finite; a program needn't handle non-finite values.
Results may differ from the reference program's by a relative error of at most 0.0029.
Values may be sent and summed in bfloat16 or wider, within the bound.
A program may use at most 64 MiB of HBM per device.

```python
import jax
import jax.numpy as jnp
from jax import lax

NB = 512
ROW_DEV = 2048
ROWS = 8192
COLS = 3072
N_PROW = 4


def draw_pivots(key, part):
    first_key, second_key, third_key = jax.random.split(key, 3)
    weights = jax.random.randint(first_key, (N_PROW,), 1, 9)
    cumulative = jnp.cumsum(weights)
    picks = jax.random.randint(second_key, (NB,), 0, cumulative[-1])
    owner = jnp.sum((picks[:, None] >= cumulative[None, :]).astype(jnp.int32), axis=1)
    onehot = (owner[:, None] == jnp.arange(N_PROW, dtype=jnp.int32)[None, :]).astype(jnp.int32)
    ranks = jnp.sum((jnp.cumsum(onehot, axis=0) - onehot) * onehot, axis=1)
    owner_keys = jax.random.split(third_key, N_PROW)
    orders = jax.vmap(lambda k: jax.random.permutation(k, ROW_DEV))(owner_keys)
    local = orders[owner, ranks]
    return (owner * ROW_DEV + local).astype(jnp.int32)


def shard_levels(rng, extent, pieces, low, high):
    def one(position, shards_of):
        heights = jax.random.uniform(jax.random.fold_in(jax.random.fold_in(rng, 6), position), (shards_of,), jnp.float32, low / len(pieces), high / len(pieces))
        return jnp.repeat(jnp.exp(heights), extent[position] // shards_of).reshape((-1,) + (1,) * (len(extent) - position - 1))

    level = one(*pieces[0])
    for cut in pieces[1:]:
        level = level * one(*cut)
    return level


def centred(stream_key, dims, deviation, reach, shards=(), kind=jnp.bfloat16):
    entries = jax.random.normal(stream_key, dims, jnp.float32) * deviation
    if len(shards) > 0:
        entries = shard_levels(stream_key, dims, shards, -0.22, 0.18) * entries
    return jnp.clip(entries, min=-reach, max=reach).astype(kind)


def setup_inputs(seed: int = 0) -> dict:
    streams_of = jax.random.split(jax.random.key(seed), 5)
    return {
        "slab": centred(streams_of[0], (ROWS, COLS), 1.0, 6.0, ((0, 4), (1, 8))),
        "pivots": draw_pivots(jax.random.fold_in(streams_of[4], 71), 0),
        "l_top": centred(streams_of[2], (NB, NB), (4 * NB) ** -0.5, 0.125),
        "l_panel_t": centred(streams_of[3], (NB, ROWS), (4 * NB) ** -0.5, 0.125, ((0, 8), (1, 4))),
    }


def bookkeeping(pivots):
    index = jnp.arange(NB, dtype=jnp.int32)
    chosen = jnp.any(pivots[:, None] == index[None, :], axis=0)
    free = jnp.logical_not(chosen)
    free_rank = jnp.cumsum(free.astype(jnp.int32)) - 1
    far = pivots >= NB
    far_rank = jnp.cumsum(far.astype(jnp.int32)) - 1
    match = free[None, :] & (free_rank[None, :] == far_rank[:, None])
    source = jnp.sum(jnp.where(match, index[None, :], 0), axis=1).astype(jnp.int32)
    return (far, source)

def reference(slab, pivots, l_top, l_panel_t):
    total_rows = slab.shape[0]
    far, source = bookkeeping(pivots)
    target = jnp.where(far, pivots, total_rows).astype(jnp.int32)
    pivoted = slab.at[target].set(slab[source], mode='drop')
    top = slab[pivots]
    lower = jnp.tril(l_top.astype(jnp.float32), -1) + jnp.eye(NB, dtype=jnp.float32)
    upper = lax.linalg.triangular_solve(lower, top.astype(jnp.float32), left_side=True, lower=True, unit_diagonal=True)
    u_block = upper.astype(jnp.bfloat16)
    u_wide = u_block.astype(jnp.float32)
    blocks = pivoted.reshape(N_PROW, ROW_DEV, -1)
    panels = jnp.transpose(l_panel_t.reshape(NB, N_PROW, ROW_DEV), (1, 0, 2))

    def one_block(pair):
        rows_here, panel_here = pair
        product = jnp.dot(panel_here.astype(jnp.float32).T.astype(jnp.float32), u_wide.astype(jnp.float32), preferred_element_type=jnp.float32)
        return (rows_here.astype(jnp.float32) - product).astype(jnp.bfloat16)
    updated = lax.map(one_block, (blocks, panels)).reshape(total_rows, -1)
    return updated.at[:NB].set(u_block)
```

```python
import functools

import jax
import jax.numpy as jnp
from jax import lax
from jax.experimental import pallas as pl
from jax.experimental.pallas import tpu as pltpu
from jax.sharding import PartitionSpec as P

MESH = pl.DeviceIdType.MESH
F32 = jnp.float32
BF16 = jnp.bfloat16
LANES = 128


def dot(a, b):
    return jnp.dot(a, b, preferred_element_type=F32)


def iota(shape, axis):
    return lax.broadcasted_iota(jnp.int32, shape, axis)


def halves(a):
    high = a.astype(BF16)
    return high, (a - high.astype(F32)).astype(BF16)


def dot_exact_left(a, b):
    high, low = halves(b)
    return dot(a, high) + dot(a, low)


def dot_split(a, b):
    a_high, a_low = halves(a)
    b_high, b_low = halves(b)
    return dot(a_high, b_high) + (dot(a_high, b_low) + dot(a_low, b_high))


EDGES = (0, 2, 6, 10, 13, 16)


def cuts(width):
    units = width // LANES
    edges = [(units * part) // 16 * LANES for part in EDGES]
    return [(a, b - a) for a, b in zip(edges[:-1], edges[1:])]


def weave(events, work):
    plan, count = [], max(1, len(events))
    for at, event in enumerate(events):
        plan += [event] + work[at * len(work) // count:(at + 1) * len(work) // count]
    return plan


def kernel(
    n_prow, n_pcol,
    slab_hbm, pivots_hbm, l_top_hbm, panel_hbm, out_ref,
    slab_ref, pivots_ref, l_top_ref, gathered, picked, picked_in, merged, homes, pivoted, inverse_hi, inverse_lo, high,
    u_ref,
    local_sem, line_recv, cross_recv, rest_recv, sent, core_sem, chip_send, chip_recv, relay_send, relay_recv,
):
    block = l_top_ref.shape[0]
    rows, width = slab_ref.shape
    me_r = lax.axis_index("prow")
    me_c = lax.axis_index("pcol")
    chips = n_prow // 2
    chip, core = me_r // 2, me_r % 2
    peer = me_r + 1 - 2 * core
    length = n_pcol // 2
    z, x = me_c // 2, me_c % 2
    other = 1 - x
    pieces = cuts(gathered.shape[2])
    bulk = range(len(pieces) - 1)
    rest = len(pieces) - 1

    panel_copy = pltpu.make_async_copy(panel_hbm, gathered.at[me_c], local_sem.at[0])
    pivots_copy = pltpu.make_async_copy(pivots_hbm, pivots_ref, local_sem.at[1])
    slab_copy = pltpu.make_async_copy(slab_hbm, slab_ref, local_sem.at[2])
    l_top_copy = pltpu.make_async_copy(l_top_hbm, l_top_ref, local_sem.at[3])

    barrier = pltpu.get_barrier_semaphore()

    def greet(r, c):
        pl.semaphore_signal(barrier, inc=1, device_id=(r, c), device_id_type=MESH)

    greet(me_r, z * 2 + other)

    @pl.when(z > 0)
    def _():
        greet(me_r, me_c - 2)

    @pl.when(z < length - 1)
    def _():
        greet(me_r, me_c + 2)

    for step in range(1, chips):
        greet(((chip + step) % chips) * 2 + core, me_c)
    greet(peer, me_c)

    panel_copy.start()
    pivots_copy.start()
    slab_copy.start()
    l_top_copy.start()

    has_below = (z + length - 1) // length
    has_above = (2 * length - 2 - z) // length

    def strip(source, piece):
        start, size = pieces[piece]
        return gathered.at[source, :, pl.ds(start, size)]

    def send(part, send_sem, recv_sem, target):
        return pltpu.make_async_remote_copy(
            src_ref=part, dst_ref=part, send_sem=send_sem, recv_sem=recv_sem,
            device_id=(me_r, target), device_id_type=MESH,
        )

    def line(way, at, piece):
        target = me_c + 2 - 4 * way
        return send(strip(at * 2 + x, piece), sent.at[way], line_recv.at[at, piece], target)

    def line_rest(way, at, side):
        target = me_c + 2 - 4 * way
        return send(strip(at * 2 + side, rest), sent.at[2 + way], rest_recv.at[at, side], target)

    def cross(at, piece):
        return send(strip(at * 2 + x, piece), sent.at[4], cross_recv.at[piece], z * 2 + other)

    def cross_rest():
        return send(strip(me_c, rest), sent.at[5], rest_recv.at[z, x], z * 2 + other)

    def both_ways(start):
        pl.when(z < length - 1)(lambda: start(0))
        pl.when(z > 0)(lambda: start(1))

    def first_sends():
        for piece in bulk:
            both_ways(lambda way: line(way, z, piece).start())
            cross(z, piece).start()
            if piece == min(1, rest - 1):
                cross_rest().start()

    def send_rest():
        both_ways(lambda way: line_rest(way, z, x).start())

    def own_rest():
        send(strip(z * 2 + other, rest), sent.at[5], rest_recv.at[z, other], z * 2 + other).wait_recv()
        both_ways(lambda way: line_rest(way, z, other).start())

    def relay(distance, piece):
        def act():
            for way, at, reached, onward in (
                (0, z - distance, z >= distance, z < length - 1),
                (1, z + distance, z < length - distance, z > 0),
            ):
                @pl.when(reached)
                def _():
                    line(way, at, piece).wait_recv()
                    pl.when(onward)(lambda: line(way, at, piece).start())
                    cross(at, piece).start()
        return act

    def relay_rest(distance):
        def act():
            for way, at, reached in (
                (0, z - distance, (z >= distance) & (z < length - 1)),
                (1, z + distance, (z < length - distance) & (z > 0)),
            ):
                @pl.when(reached)
                def _():
                    for side in (0, 1):
                        line_rest(way, at, side).wait_recv()
                        line_rest(way, at, side).start()
        return act

    def last_rests():
        for distance in range(1, length):
            for way, at, reached in (
                (0, z - distance, (z >= distance) & (z == length - 1)),
                (1, z + distance, (z < length - distance) & (z == 0)),
            ):
                @pl.when(reached)
                def _():
                    for side in (0, 1):
                        line_rest(way, at, side).wait_recv()

    def crossed(piece):
        start, size = pieces[piece]
        every = gathered.at[pl.ds(0, length), :, pl.ds(start, size)]
        send(every, sent.at[4], cross_recv.at[piece], z * 2 + other).wait_recv()

    def drain():
        wide = sum(pieces[piece][1] for piece in bulk)
        thin = pieces[rest][1]

        def gone(sem, count, size):
            part = gathered.at[pl.ds(0, count), :, pl.ds(0, size)]
            send(part, sent.at[sem], rest_recv.at[0, 0], z * 2 + other).wait_send()

        def gone_line(way, count):
            gone(way, count, wide)
            gone(2 + way, count, 2 * thin)

        for at in range(length):
            if at < length - 1:
                pl.when(z == at)(lambda: gone_line(0, at + 1))
            if at > 0:
                pl.when(z == at)(lambda: gone_line(1, length - at))
        gone(4, length, wide)
        gone(5, 1, thin)

    state = {}
    ii = iota((block, block), 0)
    jj = iota((block, block), 1)

    def column(row):
        return jnp.sum(jnp.where(ii == jj, row, 0.0), axis=1, keepdims=True)

    def bookkeeping():
        pivots_copy.wait()
        pivot_row = pivots_ref[...].astype(F32)
        pivot_col = column(pivot_row)
        chosen = jnp.max(jnp.where(pivot_col == jj.astype(F32), 1.0, 0.0), axis=0, keepdims=True)
        free = 1.0 - chosen
        far = jnp.where(pivot_row >= block, 1.0, 0.0)
        which = iota((16, block), 0)
        both = jnp.where(which == 0, free, jnp.where(which == 1, far, 0.0))
        ranks = dot(both.astype(BF16), jnp.where(ii < jj, 1.0, 0.0).astype(BF16))
        far_rank = column(ranks[1:2])
        match = (free > 0.5) & (ranks[0:1] == far_rank)
        source = jnp.sum(jnp.where(match, jj.astype(F32), 0.0), axis=1, keepdims=True)
        state.update(pivot_row=pivot_row, pivot_col=pivot_col, source=source)

    def pick():
        pivot_col, source = state["pivot_col"], state["source"]
        first = (me_r * rows).astype(F32)
        mine = (pivot_col >= first) & (pivot_col < first + rows)
        lead = (me_r == 0).astype(F32)
        index = jnp.where(mine, pivot_col - first, source * lead - (1.0 - lead))
        slab_copy.wait()
        total = jnp.zeros((block, width), F32)
        for start in range(0, rows, block):
            hot = jnp.where((jj + start).astype(F32) == index, 1.0, 0.0).astype(BF16)
            total = total + dot(hot, slab_ref[start:start + block, :])
        picked[...] = total.astype(BF16)

    def core_copy():
        return pltpu.make_async_remote_copy(
            src_ref=picked, dst_ref=picked_in, send_sem=core_sem.at[0], recv_sem=core_sem.at[1],
            device_id=(peer, me_c), device_id_type=MESH,
        )

    def own_homes():
        homes[:, width:] = jnp.ones((block, LANES), BF16)

        @pl.when(me_r == 0)
        def _():
            hot = jnp.where(jj.astype(F32) == state["source"], 1.0, 0.0).astype(BF16)
            homes[:, :width] = dot(hot, slab_ref[:block, :]).astype(BF16)

    half = block // 2

    def chip_copy(step):
        rows_of = pl.ds(pl.multiple_of(core * half, half), half)
        to = ((chip + step) % chips) * 2 + core
        return pltpu.make_async_remote_copy(
            src_ref=merged.at[0, rows_of], dst_ref=merged.at[step, rows_of],
            send_sem=chip_send.at[step - 1], recv_sem=chip_recv.at[step - 1],
            device_id=(to, me_c), device_id_type=MESH,
        )

    def relay_copy(step):
        part = merged.at[step, pl.ds(pl.multiple_of(core * half, half), half)]
        return pltpu.make_async_remote_copy(
            src_ref=part, dst_ref=part, send_sem=relay_send.at[step - 1], recv_sem=relay_recv.at[step - 1],
            device_id=(peer, me_c), device_id_type=MESH,
        )

    def merge():
        core_copy().wait()
        pivot_col = state["pivot_col"]
        lead = (chip == 0).astype(F32)
        second = jnp.where((pivot_col >= rows) & (pivot_col < 2 * rows), lead, 0.0)
        mine, theirs = picked[...].astype(F32), picked_in[...].astype(F32)
        even = (core == 0).astype(F32)
        keep_mine = 1.0 - even * second
        keep_theirs = 1.0 - (1.0 - even) * second
        merged[0] = (mine * keep_mine + theirs * keep_theirs).astype(BF16)
        for step in range(1, chips):
            chip_copy(step).start()

    def relay_chips():
        for step in range(1, chips):
            chip_copy(step).wait()
            relay_copy(step).start()

    def assemble():
        for step in range(1, chips):
            relay_copy(step).wait()
        pivot_col = state["pivot_col"]
        top = jnp.zeros((block, width), F32)
        for step in range(chips):
            low = (((chip + chips - step) % chips) * 2 * rows).astype(F32)
            here = (pivot_col >= low) & (pivot_col < low + 2 * rows)
            top = top + jnp.where(here, merged[step].astype(F32), 0.0)
        state["top"] = top.astype(BF16)

        @pl.when(me_r == 1)
        def _():
            homes[:, :width] = picked_in[...]

        for step in range(1, chips):
            @pl.when((chip > 0) & (chip == step))
            def _():
                homes[:, :width] = merged[step]

    def interchange(start):
        def act():
            row = iota((block, block), 0) + (me_r * rows + start)
            pivot_row = state["pivot_row"]
            hot = jnp.where((row.astype(F32) == pivot_row) & (pivot_row >= block), 1.0, 0.0)
            both = dot(hot.astype(BF16), homes[...])
            taken = both[:, width:] > 0.5
            for lane in range(0, width, LANES):
                kept = slab_ref[start:start + block, lane:lane + LANES].astype(F32)
                new = jnp.where(taken, both[:, lane:lane + LANES], kept)
                pivoted[start:start + block, lane:lane + LANES] = new.astype(BF16)
        return act

    base = min(block, 256)
    small = min(base, 16)
    bi = iota((base, base), 0)
    bj = iota((base, base), 1)
    groups = block // base

    def diagonal(g):
        part = l_top_ref[g * base:(g + 1) * base, g * base:(g + 1) * base].astype(F32)
        return jnp.where(bi > bj, part, 0.0)

    def start_inverse():
        l_top_copy.wait()
        state["x"], state["power"] = [], []
        for g in range(groups):
            near = jnp.where(bi // small == bj // small, diagonal(g), 0.0)
            state["x"].append(jnp.where(bi == bj, 1.0, 0.0) - near)
            exact = near.astype(BF16)
            state["power"].append(dot(exact, exact))

    def power_step():
        for g in range(groups):
            x, power = state["x"][g], state["power"][g]
            state["x"][g] = x + dot_split(x, power)
            state["power"][g] = dot_split(power, power)

    def last_power():
        for g in range(groups):
            x, power = state["x"][g], state["power"][g]
            state["x"][g] = x + dot_split(x, power)

    def double(size):
        def act():
            for g in range(groups):
                link = jnp.where(
                    (bi // (2 * size) == bj // (2 * size)) & (bi // size != bj // size), diagonal(g), 0.0
                )
                inv = state["x"][g]
                state["x"][g] = inv - dot_split(inv, dot_exact_left(link.astype(BF16), inv))
        return act

    def join():
        for g in range(groups):
            high[g * base:(g + 1) * base, :] = jnp.zeros((base, block), F32)
            high[g * base:(g + 1) * base, g * base:(g + 1) * base] = state["x"][g]

    def join_double(size):
        def act():
            for at in range(0, block, 2 * size):
                a = high[at:at + size, at:at + size]
                b = high[at + size:at + 2 * size, at + size:at + 2 * size]
                c = l_top_ref[at + size:at + 2 * size, at:at + size]
                high[at + size:at + 2 * size, at:at + size] = -dot_split(b, dot_exact_left(c, a))
        return act

    def split():
        inverse_hi[...], inverse_lo[...] = halves(high[...])

    def solve():
        top = state["top"]
        u_ref[...] = (dot(inverse_hi[...], top) + dot(inverse_lo[...], top)).astype(BF16)

    inverse = [start_inverse]
    size = 4
    while size < small:
        inverse.append(power_step)
        size *= 2
    if small > 2:
        inverse.append(last_power)
    size = small
    while size < base:
        inverse.append(double(size))
        size *= 2
    inverse.append(join)
    while size < block:
        inverse.append(join_double(size))
        size *= 2
    inverse.append(split)

    def update(piece):
        start, size = pieces[piece]
        panel = gathered[:, :, start:start + size].reshape(block, size).astype(BF16)
        product = lax.dot_general(
            panel, u_ref[...], (((0,), (0,)), ((), ())), preferred_element_type=F32
        )
        out_ref[start:start + size, :] = (pivoted[start:start + size, :].astype(F32) - product).astype(BF16)

    pl.semaphore_wait(barrier, 1 + chips + has_below + has_above)
    panel_copy.wait()
    pl.when(core == 0)(first_sends)
    bookkeeping()
    pick()
    core_copy().start()
    pl.when(core == 1)(first_sends)
    own_homes()

    def relays(distance):
        return [relay(distance, piece) for piece in bulk] if distance < length else []

    changes = [interchange(start) for start in range(0, rows, block)]
    plan = inverse[:3] + [merge] + weave(relays(1), [send_rest] + inverse[3:6]) + [own_rest] + inverse[6:8]
    plan += weave(relays(2), inverse[8:10] + [relay_chips] + inverse[10:]) + [relay_rest(1), assemble, solve]
    plan += weave(relays(3), changes[:3] + [relay_rest(2)]) + changes[3:]
    for distance in range(4, length):
        plan += relays(distance) + [relay_rest(distance - 1)]
    plan += [relay_rest(length - 1)]
    for act in plan:
        act()

    for piece in bulk:
        crossed(piece)
        update(piece)
    last_rests()
    update(rest)

    @pl.when(me_r == 0)
    def _():
        out_ref[:block, :] = u_ref[...]

    drain()


def per_device(n_prow, n_pcol, slab, pivots, l_top, l_panel_t):
    rows, width = slab.shape
    block = pivots.shape[0]
    depth = l_panel_t.shape[0]
    kind = BF16 if depth % 16 == 0 else F32
    panel = l_panel_t.astype(kind)
    chips = n_prow // 2
    n_pieces = len(cuts(rows))
    vmem = pl.BlockSpec(memory_space=pltpu.VMEM)
    anywhere = pl.BlockSpec(memory_space=pltpu.HBM)
    dma = pltpu.SemaphoreType.DMA
    return pl.pallas_call(
        functools.partial(kernel, n_prow, n_pcol),
        out_shape=pltpu.VMEM((rows, width), BF16),
        in_specs=[anywhere] * 4,
        out_specs=vmem,
        scratch_shapes=[
            pltpu.VMEM((rows, width), BF16),
            pltpu.VMEM((1, block), jnp.int32),
            pltpu.VMEM((block, block), BF16),
            pltpu.VMEM((n_pcol, depth, rows), kind),
            pltpu.VMEM((block, width), BF16),
            pltpu.VMEM((block, width), BF16),
            pltpu.VMEM((chips, block, width), BF16),
            pltpu.VMEM((block, width + LANES), BF16),
            pltpu.VMEM((rows, width), BF16),
            pltpu.VMEM((block, block), BF16),
            pltpu.VMEM((block, block), BF16),
            pltpu.VMEM((block, block), F32),
            pltpu.VMEM((block, width), BF16),
            dma((4,)),
            dma((n_pcol // 2, n_pieces - 1)),
            dma((n_pieces - 1,)),
            dma((n_pcol // 2, 2)),
            dma((6,)),
            dma((2,)),
            dma((chips - 1,)),
            dma((chips - 1,)),
            dma((chips - 1,)),
            dma((chips - 1,)),
        ],
        compiler_params=pltpu.CompilerParams(collective_id=0, has_side_effects=True, vmem_limit_bytes=60 * 2**20),
    )(slab, pivots.reshape(1, block), l_top, panel)


def solution(mesh):
    return jax.shard_map(
        functools.partial(per_device, mesh.shape["prow"], mesh.shape["pcol"]),
        mesh=mesh,
        in_specs=(P("prow", "pcol"), P(), P(), P("pcol", "prow")),
        out_specs=P("prow", "pcol"),
        check_vma=False,
    )
```

```python
import functools

import jax
import jax.numpy as jnp
from jax import lax
from jax.experimental import pallas as pl
from jax.experimental.pallas import tpu as pltpu
from jax.sharding import PartitionSpec as P

MESH = pl.DeviceIdType.MESH
F32 = jnp.float32
BF16 = jnp.bfloat16
LANES = 128


def dot(a, b):
    return jnp.dot(a, b, preferred_element_type=F32)


def iota(shape, axis):
    return lax.broadcasted_iota(jnp.int32, shape, axis)


def halves(a):
    high = a.astype(BF16)
    return high, (a - high.astype(F32)).astype(BF16)


def dot_exact_left(a, b):
    high, low = halves(b)
    return dot(a, high) + dot(a, low)


def dot_split(a, b):
    a_high, a_low = halves(a)
    b_high, b_low = halves(b)
    return dot(a_high, b_high) + (dot(a_high, b_low) + dot(a_low, b_high))


EDGES = (0, 4, 8, 11, 13, 16)


def cuts(width):
    units = width // LANES
    edges = [(units * part) // 16 * LANES for part in EDGES]
    return [(a, b - a) for a, b in zip(edges[:-1], edges[1:])]


def weave(events, work):
    plan, count = [], max(1, len(events))
    for at, event in enumerate(events):
        plan += [event] + work[at * len(work) // count:(at + 1) * len(work) // count]
    return plan


def kernel(
    n_prow, n_pcol,
    slab_hbm, pivots_hbm, l_top_hbm, panel_hbm, out_ref,
    slab_ref, pivots_ref, l_top_ref, gathered, picked, picked_in, merged, homes, pivoted, inverse_hi, inverse_lo, high,
    u_ref,
    local_sem, line_recv, cross_recv, rest_recv, sent, core_sem, chip_send, chip_recv, relay_send, relay_recv,
):
    block = l_top_ref.shape[0]
    rows, width = slab_ref.shape
    me_r = lax.axis_index("prow")
    me_c = lax.axis_index("pcol")
    chips = n_prow // 2
    chip, core = me_r // 2, me_r % 2
    peer = me_r + 1 - 2 * core
    length = n_pcol // 2
    z, x = me_c // 2, me_c % 2
    other = 1 - x
    pieces = cuts(gathered.shape[2])
    bulk = range(len(pieces) - 1)
    rest = len(pieces) - 1
    lead = me_r == 0

    def needed(piece, act):
        start, size = pieces[piece]
        if start + size <= block:
            pl.when(jnp.logical_not(lead))(act)
        else:
            act()

    panel_copy = pltpu.make_async_copy(panel_hbm, gathered.at[me_c], local_sem.at[0])
    pivots_copy = pltpu.make_async_copy(pivots_hbm, pivots_ref, local_sem.at[1])
    slab_copy = pltpu.make_async_copy(slab_hbm, slab_ref, local_sem.at[2])
    l_top_copy = pltpu.make_async_copy(l_top_hbm, l_top_ref, local_sem.at[3])

    barrier = pltpu.get_barrier_semaphore()

    def greet(r, c):
        pl.semaphore_signal(barrier, inc=1, device_id=(r, c), device_id_type=MESH)

    greet(me_r, z * 2 + other)

    @pl.when(z > 0)
    def _():
        greet(me_r, me_c - 2)

    @pl.when(z < length - 1)
    def _():
        greet(me_r, me_c + 2)

    for step in range(1, chips):
        greet(((chip + step) % chips) * 2 + core, me_c)
    greet(peer, me_c)

    panel_copy.start()
    pivots_copy.start()
    slab_copy.start()
    l_top_copy.start()

    has_below = (z + length - 1) // length
    has_above = (2 * length - 2 - z) // length

    def strip(source, piece):
        start, size = pieces[piece]
        return gathered.at[source, :, pl.ds(start, size)]

    def send(part, send_sem, recv_sem, target):
        return pltpu.make_async_remote_copy(
            src_ref=part, dst_ref=part, send_sem=send_sem, recv_sem=recv_sem,
            device_id=(me_r, target), device_id_type=MESH,
        )

    def line(way, at, piece):
        target = me_c + 2 - 4 * way
        return send(strip(at * 2 + x, piece), sent.at[way], line_recv.at[at, piece], target)

    def line_rest(way, at, side):
        target = me_c + 2 - 4 * way
        return send(strip(at * 2 + side, rest), sent.at[2 + way], rest_recv.at[at, side], target)

    def cross(at, piece):
        return send(strip(at * 2 + x, piece), sent.at[4], cross_recv.at[piece], z * 2 + other)

    def cross_rest():
        return send(strip(me_c, rest), sent.at[5], rest_recv.at[z, x], z * 2 + other)

    def both_ways(start):
        pl.when(z < length - 1)(lambda: start(0))
        pl.when(z > 0)(lambda: start(1))

    def first_sends():
        for piece in bulk:
            def own():
                both_ways(lambda way: line(way, z, piece).start())
                cross(z, piece).start()
            needed(piece, own)
            if piece == rest // 2:
                cross_rest().start()
        own_rest(0, x)()

    def rest_ways(distance, act):
        if distance < length - 1:
            pl.when(z == distance)(lambda: act(0))
            pl.when(z == length - 1 - distance)(lambda: act(1))

    def own_rest(distance, side):
        return lambda: rest_ways(distance, lambda way: line_rest(way, z, side).start())

    def other_rest():
        send(strip(z * 2 + other, rest), sent.at[5], rest_recv.at[z, other], z * 2 + other).wait_recv()

    def pass_rest(distance, reach):
        def onward(way):
            at = z + (2 * way - 1) * reach
            for side in (0, 1):
                line_rest(way, at, side).wait_recv()
                line_rest(way, at, side).start()
        return lambda: rest_ways(distance, onward)

    def relay(distance, piece):
        def both():
            for way, at, reached, onward in (
                (0, z - distance, z >= distance, z < length - 1),
                (1, z + distance, z < length - distance, z > 0),
            ):
                @pl.when(reached)
                def _():
                    line(way, at, piece).wait_recv()
                    pl.when(onward)(lambda: line(way, at, piece).start())
                    cross(at, piece).start()
        return lambda: needed(piece, both)

    def last_rests():
        for distance in range(1, length):
            for way, at, reached in (
                (0, z - distance, (z >= distance) & (z == length - 1)),
                (1, z + distance, (z < length - distance) & (z == 0)),
            ):
                @pl.when(reached)
                def _():
                    for side in (0, 1):
                        line_rest(way, at, side).wait_recv()

    def crossed(piece):
        start, size = pieces[piece]
        every = gathered.at[pl.ds(0, length), :, pl.ds(start, size)]
        needed(piece, lambda: send(every, sent.at[4], cross_recv.at[piece], z * 2 + other).wait_recv())

    def drain():
        thin = pieces[rest][1]

        def gone(sem, count, size):
            part = gathered.at[pl.ds(0, count), :, pl.ds(0, size)]
            send(part, sent.at[sem], rest_recv.at[0, 0], z * 2 + other).wait_send()

        def gone_bulk(sem, count):
            def wide(first):
                return sum(size for start, size in pieces[:-1] if start + size > first)

            pl.when(lead)(lambda: gone(sem, count, wide(block)))
            pl.when(jnp.logical_not(lead))(lambda: gone(sem, count, wide(0)))

        def gone_line(way, count):
            gone_bulk(way, count)
            gone(2 + way, count, 2 * thin)

        for at in range(length):
            if at < length - 1:
                pl.when(z == at)(lambda: gone_line(0, at + 1))
            if at > 0:
                pl.when(z == at)(lambda: gone_line(1, length - at))
        gone_bulk(4, length)
        gone(5, 1, thin)

    state = {}
    ii = iota((block, block), 0)
    jj = iota((block, block), 1)

    def column(row):
        return jnp.sum(jnp.where(ii == jj, row, 0.0), axis=1, keepdims=True)

    def bookkeeping():
        pivots_copy.wait()
        pivot_row = pivots_ref[...].astype(F32)
        pivot_col = column(pivot_row)
        chosen = jnp.max(jnp.where(pivot_col == jj.astype(F32), 1.0, 0.0), axis=0, keepdims=True)
        free = 1.0 - chosen
        far = jnp.where(pivot_row >= block, 1.0, 0.0)
        which = iota((16, block), 0)
        both = jnp.where(which == 0, free, jnp.where(which == 1, far, 0.0))
        ranks = dot(both.astype(BF16), jnp.where(ii < jj, 1.0, 0.0).astype(BF16))
        far_rank = column(ranks[1:2])
        match = (free > 0.5) & (ranks[0:1] == far_rank)
        source = jnp.sum(jnp.where(match, jj.astype(F32), 0.0), axis=1, keepdims=True)
        state.update(pivot_row=pivot_row, pivot_col=pivot_col, source=source)

    def pick():
        pivot_col, source = state["pivot_col"], state["source"]
        first = (me_r * rows).astype(F32)
        mine = (pivot_col >= first) & (pivot_col < first + rows)
        holds = lead.astype(F32)
        index = jnp.where(mine, pivot_col - first, source * holds - (1.0 - holds))
        slab_copy.wait()
        total = jnp.zeros((block, width), F32)
        for start in range(0, rows, block):
            hot = jnp.where((jj + start).astype(F32) == index, 1.0, 0.0).astype(BF16)
            total = total + dot(hot, slab_ref[start:start + block, :])
        picked[...] = total.astype(BF16)

    def core_copy():
        return pltpu.make_async_remote_copy(
            src_ref=picked, dst_ref=picked_in, send_sem=core_sem.at[0], recv_sem=core_sem.at[1],
            device_id=(peer, me_c), device_id_type=MESH,
        )

    def own_homes():
        homes[:, width:] = jnp.ones((block, LANES), BF16)

        @pl.when(me_r == 0)
        def _():
            hot = jnp.where(jj.astype(F32) == state["source"], 1.0, 0.0).astype(BF16)
            homes[:, :width] = dot(hot, slab_ref[:block, :]).astype(BF16)

    half = block // 2

    def chip_copy(step):
        rows_of = pl.ds(pl.multiple_of(core * half, half), half)
        to = ((chip + step) % chips) * 2 + core
        return pltpu.make_async_remote_copy(
            src_ref=merged.at[0, rows_of], dst_ref=merged.at[step, rows_of],
            send_sem=chip_send.at[step - 1], recv_sem=chip_recv.at[step - 1],
            device_id=(to, me_c), device_id_type=MESH,
        )

    def relay_copy(step):
        part = merged.at[step, pl.ds(pl.multiple_of(core * half, half), half)]
        return pltpu.make_async_remote_copy(
            src_ref=part, dst_ref=part, send_sem=relay_send.at[step - 1], recv_sem=relay_recv.at[step - 1],
            device_id=(peer, me_c), device_id_type=MESH,
        )

    def merge():
        core_copy().wait()
        pivot_col = state["pivot_col"]
        holds = (chip == 0).astype(F32)
        second = jnp.where((pivot_col >= rows) & (pivot_col < 2 * rows), holds, 0.0)
        mine, theirs = picked[...].astype(F32), picked_in[...].astype(F32)
        even = (core == 0).astype(F32)
        keep_mine = 1.0 - even * second
        keep_theirs = 1.0 - (1.0 - even) * second
        merged[0] = (mine * keep_mine + theirs * keep_theirs).astype(BF16)
        for step in range(1, chips):
            chip_copy(step).start()

    def relay_chips():
        for step in range(1, chips):
            chip_copy(step).wait()
            relay_copy(step).start()

    def assemble():
        for step in range(1, chips):
            relay_copy(step).wait()
        pivot_col = state["pivot_col"]
        top = jnp.zeros((block, width), F32)
        for step in range(chips):
            low = (((chip + chips - step) % chips) * 2 * rows).astype(F32)
            here = (pivot_col >= low) & (pivot_col < low + 2 * rows)
            top = top + jnp.where(here, merged[step].astype(F32), 0.0)
        state["top"] = top.astype(BF16)

        @pl.when(me_r == 1)
        def _():
            homes[:, :width] = picked_in[...]

        for step in range(1, chips):
            @pl.when((chip > 0) & (chip == step))
            def _():
                homes[:, :width] = merged[step]

    def interchange(start):
        def act():
            row = iota((block, block), 0) + (me_r * rows + start)
            pivot_row = state["pivot_row"]
            hot = jnp.where((row.astype(F32) == pivot_row) & (pivot_row >= block), 1.0, 0.0)
            both = dot(hot.astype(BF16), homes[...])
            taken = both[:, width:] > 0.5
            for lane in range(0, width, LANES):
                kept = slab_ref[start:start + block, lane:lane + LANES].astype(F32)
                new = jnp.where(taken, both[:, lane:lane + LANES], kept)
                pivoted[start:start + block, lane:lane + LANES] = new.astype(BF16)
        return act

    base = min(block, 256)
    small = min(base, 16)
    bi = iota((base, base), 0)
    bj = iota((base, base), 1)
    groups = block // base

    def diagonal(g):
        part = l_top_ref[g * base:(g + 1) * base, g * base:(g + 1) * base].astype(F32)
        return jnp.where(bi > bj, part, 0.0)

    def start_inverse():
        l_top_copy.wait()
        state["x"], state["power"] = [], []
        for g in range(groups):
            near = jnp.where(bi // small == bj // small, diagonal(g), 0.0)
            state["x"].append(jnp.where(bi == bj, 1.0, 0.0) - near)
            exact = near.astype(BF16)
            state["power"].append(dot(exact, exact))

    def power_step():
        for g in range(groups):
            x, power = state["x"][g], state["power"][g]
            state["x"][g] = x + dot_split(x, power)
            state["power"][g] = dot_split(power, power)

    def last_power():
        for g in range(groups):
            x, power = state["x"][g], state["power"][g]
            state["x"][g] = x + dot_split(x, power)

    def double(size):
        def act():
            for g in range(groups):
                link = jnp.where(
                    (bi // (2 * size) == bj // (2 * size)) & (bi // size != bj // size), diagonal(g), 0.0
                )
                inv = state["x"][g]
                state["x"][g] = inv - dot_split(inv, dot_exact_left(link.astype(BF16), inv))
        return act

    def join():
        for g in range(groups):
            high[g * base:(g + 1) * base, :] = jnp.zeros((base, block), F32)
            high[g * base:(g + 1) * base, g * base:(g + 1) * base] = state["x"][g]

    def join_double(size):
        def act():
            for at in range(0, block, 2 * size):
                a = high[at:at + size, at:at + size]
                b = high[at + size:at + 2 * size, at + size:at + 2 * size]
                c = l_top_ref[at + size:at + 2 * size, at:at + size]
                high[at + size:at + 2 * size, at:at + size] = -dot_split(b, dot_exact_left(c, a))
        return act

    def split():
        inverse_hi[...], inverse_lo[...] = halves(high[...])

    def solve():
        top = state["top"]
        u_ref[...] = (dot(inverse_hi[...], top) + dot(inverse_lo[...], top)).astype(BF16)

    inverse = [start_inverse]
    size = 4
    while size < small:
        inverse.append(power_step)
        size *= 2
    if small > 2:
        inverse.append(last_power)
    size = small
    while size < base:
        inverse.append(double(size))
        size *= 2
    inverse.append(join)
    while size < block:
        inverse.append(join_double(size))
        size *= 2
    inverse.append(split)

    def update(piece):
        start, size = pieces[piece]

        def act():
            panel = gathered[:, :, start:start + size].reshape(block, size).astype(BF16)
            product = lax.dot_general(
                panel, u_ref[...], (((0,), (0,)), ((), ())), preferred_element_type=F32
            )
            out_ref[start:start + size, :] = (pivoted[start:start + size, :].astype(F32) - product).astype(BF16)

        needed(piece, act)
        if start < block:
            @pl.when(lead)
            def _():
                end = min(block, start + size)
                out_ref[start:end, :] = u_ref[start:end, :]

    pl.semaphore_wait(barrier, 1 + chips + has_below + has_above)
    panel_copy.wait()
    first_sends()
    bookkeeping()
    pick()
    core_copy().start()

    own_homes()

    def relays(distance):
        return [relay(distance, piece) for piece in bulk] if distance < length else []

    changes = [interchange(start) for start in range(0, rows, block)]
    plan = inverse[:3] + [merge] + weave(relays(1), inverse[3:6])
    plan += [other_rest, own_rest(0, other), own_rest(1, x), own_rest(1, other)] + inverse[6:8]
    second = relays(2)
    half_way = len(second) // 2
    plan += weave(second[:half_way], inverse[8:10]) + [pass_rest(1, 1)]
    plan += weave(second[half_way:], [relay_chips] + inverse[10:])
    plan += [own_rest(2, x), own_rest(2, other), pass_rest(2, 1), assemble, solve]
    plan += weave(relays(3), changes[:3] + [pass_rest(2, 2)]) + changes[3:]
    for distance in range(3, length):
        plan += relays(distance) if distance > 3 else []
        plan += [own_rest(distance, x), own_rest(distance, other)]
        plan += [pass_rest(distance, reach) for reach in range(1, distance + 1)]
    for act in plan:
        act()

    for piece in bulk:
        crossed(piece)
        update(piece)
    last_rests()
    update(rest)

    drain()


def per_device(n_prow, n_pcol, slab, pivots, l_top, l_panel_t):
    rows, width = slab.shape
    block = pivots.shape[0]
    depth = l_panel_t.shape[0]
    kind = BF16 if depth % 16 == 0 else F32
    panel = l_panel_t.astype(kind)
    chips = n_prow // 2
    n_pieces = len(cuts(rows))
    vmem = pl.BlockSpec(memory_space=pltpu.VMEM)
    anywhere = pl.BlockSpec(memory_space=pltpu.HBM)
    dma = pltpu.SemaphoreType.DMA
    return pl.pallas_call(
        functools.partial(kernel, n_prow, n_pcol),
        out_shape=pltpu.VMEM((rows, width), BF16),
        in_specs=[anywhere] * 4,
        out_specs=vmem,
        scratch_shapes=[
            pltpu.VMEM((rows, width), BF16),
            pltpu.VMEM((1, block), jnp.int32),
            pltpu.VMEM((block, block), BF16),
            pltpu.VMEM((n_pcol, depth, rows), kind),
            pltpu.VMEM((block, width), BF16),
            pltpu.VMEM((block, width), BF16),
            pltpu.VMEM((chips, block, width), BF16),
            pltpu.VMEM((block, width + LANES), BF16),
            pltpu.VMEM((rows, width), BF16),
            pltpu.VMEM((block, block), BF16),
            pltpu.VMEM((block, block), BF16),
            pltpu.VMEM((block, block), F32),
            pltpu.VMEM((block, width), BF16),
            dma((4,)),
            dma((n_pcol // 2, n_pieces - 1)),
            dma((n_pieces - 1,)),
            dma((n_pcol // 2, 2)),
            dma((6,)),
            dma((2,)),
            dma((chips - 1,)),
            dma((chips - 1,)),
            dma((chips - 1,)),
            dma((chips - 1,)),
        ],
        compiler_params=pltpu.CompilerParams(collective_id=0, has_side_effects=True, vmem_limit_bytes=60 * 2**20),
    )(slab, pivots.reshape(1, block), l_top, panel)


def solution(mesh):
    return jax.shard_map(
        functools.partial(per_device, mesh.shape["prow"], mesh.shape["pcol"]),
        mesh=mesh,
        in_specs=(P("prow", "pcol"), P(), P(), P("pcol", "prow")),
        out_specs=P("prow", "pcol"),
        check_vma=False,
    )
```

```python
import functools

import jax
import jax.numpy as jnp
from jax import lax
from jax.experimental import pallas as pl
from jax.experimental.pallas import tpu as pltpu
from jax.sharding import PartitionSpec as P

MESH = pl.DeviceIdType.MESH
F32 = jnp.float32
BF16 = jnp.bfloat16
LANES = 128


def dot(a, b):
    return jnp.dot(a, b, preferred_element_type=F32)


def iota(shape, axis):
    return lax.broadcasted_iota(jnp.int32, shape, axis)


def halves(a):
    high = a.astype(BF16)
    return high, (a - high.astype(F32)).astype(BF16)


def dot_exact_left(a, b):
    high, low = halves(b)
    return dot(a, high) + dot(a, low)


def dot_split(a, b):
    a_high, a_low = halves(a)
    b_high, b_low = halves(b)
    return dot(a_high, b_high) + (dot(a_high, b_low) + dot(a_low, b_high))


EDGES = (0, 4, 8, 11, 13, 16)
LATE = 3
LIMIT = 54 * 2**20


def cuts(width):
    units = width // LANES
    edges = [(units * part) // 16 * LANES for part in EDGES]
    return [(a, b - a) for a, b in zip(edges[:-1], edges[1:])]


def weave(events, work):
    plan, count = [], max(1, len(events))
    for at, event in enumerate(events):
        plan += [event] + work[at * len(work) // count:(at + 1) * len(work) // count]
    return plan


def late_pieces(block, width):
    pieces = cuts(width)
    return [piece for piece in range(LATE, len(pieces)) if pieces[piece][0] >= block]


def trailing(panel, u, rows):
    product = lax.dot_general(panel, u, (((0,), (0,)), ((), ())), preferred_element_type=F32)
    return (rows.astype(F32) - product).astype(BF16)


def kernel(
    n_prow, n_pcol,
    slab_hbm, pivots_hbm, l_top_hbm, panel_hbm, out_ref, gathered, pivoted, u_ref,
    slab_ref, pivots_ref, l_top_ref, picked, picked_in, merged, homes, inverse_hi, inverse_lo, high,
    local_sem, line_recv, cross_recv, rest_recv, sent, core_sem, chip_send, chip_recv, relay_send, relay_recv,
):
    block = l_top_ref.shape[0]
    rows, width = slab_ref.shape
    me_r = lax.axis_index("prow")
    me_c = lax.axis_index("pcol")
    chips = n_prow // 2
    chip, core = me_r // 2, me_r % 2
    peer = me_r + 1 - 2 * core
    length = n_pcol // 2
    z, x = me_c // 2, me_c % 2
    other = 1 - x
    pieces = cuts(gathered.shape[2])
    bulk = range(len(pieces) - 1)
    rest = len(pieces) - 1
    lead = me_r == 0

    def needed(piece, act):
        start, size = pieces[piece]
        if start + size <= block:
            pl.when(jnp.logical_not(lead))(act)
        else:
            act()

    panel_copy = pltpu.make_async_copy(panel_hbm, gathered.at[me_c], local_sem.at[0])
    pivots_copy = pltpu.make_async_copy(pivots_hbm, pivots_ref, local_sem.at[1])
    slab_copy = pltpu.make_async_copy(slab_hbm, slab_ref, local_sem.at[2])
    l_top_copy = pltpu.make_async_copy(l_top_hbm, l_top_ref, local_sem.at[3])

    barrier = pltpu.get_barrier_semaphore()

    def greet(r, c):
        pl.semaphore_signal(barrier, inc=1, device_id=(r, c), device_id_type=MESH)

    greet(me_r, z * 2 + other)

    @pl.when(z > 0)
    def _():
        greet(me_r, me_c - 2)

    @pl.when(z < length - 1)
    def _():
        greet(me_r, me_c + 2)

    for step in range(1, chips):
        greet(((chip + step) % chips) * 2 + core, me_c)
    greet(peer, me_c)

    panel_copy.start()
    pivots_copy.start()
    slab_copy.start()
    l_top_copy.start()

    has_below = (z + length - 1) // length
    has_above = (2 * length - 2 - z) // length

    def strip(source, piece):
        start, size = pieces[piece]
        return gathered.at[source, :, pl.ds(start, size)]

    def send(part, send_sem, recv_sem, target):
        return pltpu.make_async_remote_copy(
            src_ref=part, dst_ref=part, send_sem=send_sem, recv_sem=recv_sem,
            device_id=(me_r, target), device_id_type=MESH,
        )

    def line(way, at, piece):
        target = me_c + 2 - 4 * way
        return send(strip(at * 2 + x, piece), sent.at[way], line_recv.at[at, piece], target)

    def line_rest(way, at, side):
        target = me_c + 2 - 4 * way
        return send(strip(at * 2 + side, rest), sent.at[2 + way], rest_recv.at[at, side], target)

    def cross(at, piece):
        return send(strip(at * 2 + x, piece), sent.at[4], cross_recv.at[piece], z * 2 + other)

    def cross_rest():
        return send(strip(me_c, rest), sent.at[5], rest_recv.at[z, x], z * 2 + other)

    def both_ways(start):
        pl.when(z < length - 1)(lambda: start(0))
        pl.when(z > 0)(lambda: start(1))

    def first_sends():
        for piece in bulk:
            def own():
                both_ways(lambda way: line(way, z, piece).start())
                cross(z, piece).start()
            needed(piece, own)
            if piece == rest // 2:
                cross_rest().start()
        own_rest(0, x)()

    def rest_ways(distance, act):
        if distance < length - 1:
            pl.when(z == distance)(lambda: act(0))
            pl.when(z == length - 1 - distance)(lambda: act(1))

    def own_rest(distance, side):
        return lambda: rest_ways(distance, lambda way: line_rest(way, z, side).start())

    def other_rest():
        send(strip(z * 2 + other, rest), sent.at[5], rest_recv.at[z, other], z * 2 + other).wait_recv()

    def pass_rest(distance, reach):
        def onward(way):
            at = z + (2 * way - 1) * reach
            for side in (0, 1):
                line_rest(way, at, side).wait_recv()
                line_rest(way, at, side).start()
        return lambda: rest_ways(distance, onward)

    def relay(distance, piece):
        def both():
            for way, at, reached, onward in (
                (0, z - distance, z >= distance, z < length - 1),
                (1, z + distance, z < length - distance, z > 0),
            ):
                @pl.when(reached)
                def _():
                    line(way, at, piece).wait_recv()
                    pl.when(onward)(lambda: line(way, at, piece).start())
                    cross(at, piece).start()
        return lambda: needed(piece, both)

    def last_rests():
        for distance in range(1, length):
            for way, at, reached in (
                (0, z - distance, (z >= distance) & (z == length - 1)),
                (1, z + distance, (z < length - distance) & (z == 0)),
            ):
                @pl.when(reached)
                def _():
                    for side in (0, 1):
                        line_rest(way, at, side).wait_recv()

    def crossed(piece):
        start, size = pieces[piece]
        every = gathered.at[pl.ds(0, length), :, pl.ds(start, size)]
        needed(piece, lambda: send(every, sent.at[4], cross_recv.at[piece], z * 2 + other).wait_recv())

    def drain():
        thin = pieces[rest][1]

        def gone(sem, count, size):
            part = gathered.at[pl.ds(0, count), :, pl.ds(0, size)]
            send(part, sent.at[sem], rest_recv.at[0, 0], z * 2 + other).wait_send()

        def gone_bulk(sem, count):
            def wide(first):
                return sum(size for start, size in pieces[:-1] if start + size > first)

            pl.when(lead)(lambda: gone(sem, count, wide(block)))
            pl.when(jnp.logical_not(lead))(lambda: gone(sem, count, wide(0)))

        def gone_line(way, count):
            gone_bulk(way, count)
            gone(2 + way, count, 2 * thin)

        for at in range(length):
            if at < length - 1:
                pl.when(z == at)(lambda: gone_line(0, at + 1))
            if at > 0:
                pl.when(z == at)(lambda: gone_line(1, length - at))
        gone_bulk(4, length)
        gone(5, 1, thin)

    state = {}
    ii = iota((block, block), 0)
    jj = iota((block, block), 1)

    def column(row):
        return jnp.sum(jnp.where(ii == jj, row, 0.0), axis=1, keepdims=True)

    def bookkeeping():
        pivots_copy.wait()
        pivot_row = pivots_ref[...].astype(F32)
        pivot_col = column(pivot_row)
        chosen = jnp.max(jnp.where(pivot_col == jj.astype(F32), 1.0, 0.0), axis=0, keepdims=True)
        free = 1.0 - chosen
        far = jnp.where(pivot_row >= block, 1.0, 0.0)
        which = iota((16, block), 0)
        both = jnp.where(which == 0, free, jnp.where(which == 1, far, 0.0))
        ranks = dot(both.astype(BF16), jnp.where(ii < jj, 1.0, 0.0).astype(BF16))
        far_rank = column(ranks[1:2])
        match = (free > 0.5) & (ranks[0:1] == far_rank)
        source = jnp.sum(jnp.where(match, jj.astype(F32), 0.0), axis=1, keepdims=True)
        state.update(pivot_row=pivot_row, pivot_col=pivot_col, source=source)

    def pick():
        pivot_col, source = state["pivot_col"], state["source"]
        first = (me_r * rows).astype(F32)
        mine = (pivot_col >= first) & (pivot_col < first + rows)
        holds = lead.astype(F32)
        index = jnp.where(mine, pivot_col - first, source * holds - (1.0 - holds))
        slab_copy.wait()
        total = jnp.zeros((block, width), F32)
        for start in range(0, rows, block):
            hot = jnp.where((jj + start).astype(F32) == index, 1.0, 0.0).astype(BF16)
            total = total + dot(hot, slab_ref[start:start + block, :])
        picked[...] = total.astype(BF16)

    def core_copy():
        return pltpu.make_async_remote_copy(
            src_ref=picked, dst_ref=picked_in, send_sem=core_sem.at[0], recv_sem=core_sem.at[1],
            device_id=(peer, me_c), device_id_type=MESH,
        )

    def own_homes():
        homes[:, width:] = jnp.ones((block, LANES), BF16)

        @pl.when(me_r == 0)
        def _():
            hot = jnp.where(jj.astype(F32) == state["source"], 1.0, 0.0).astype(BF16)
            homes[:, :width] = dot(hot, slab_ref[:block, :]).astype(BF16)

    half = block // 2

    def chip_copy(step):
        rows_of = pl.ds(pl.multiple_of(core * half, half), half)
        to = ((chip + step) % chips) * 2 + core
        return pltpu.make_async_remote_copy(
            src_ref=merged.at[0, rows_of], dst_ref=merged.at[step, rows_of],
            send_sem=chip_send.at[step - 1], recv_sem=chip_recv.at[step - 1],
            device_id=(to, me_c), device_id_type=MESH,
        )

    def relay_copy(step):
        part = merged.at[step, pl.ds(pl.multiple_of(core * half, half), half)]
        return pltpu.make_async_remote_copy(
            src_ref=part, dst_ref=part, send_sem=relay_send.at[step - 1], recv_sem=relay_recv.at[step - 1],
            device_id=(peer, me_c), device_id_type=MESH,
        )

    def merge():
        core_copy().wait()
        pivot_col = state["pivot_col"]
        holds = (chip == 0).astype(F32)
        second = jnp.where((pivot_col >= rows) & (pivot_col < 2 * rows), holds, 0.0)
        mine, theirs = picked[...].astype(F32), picked_in[...].astype(F32)
        even = (core == 0).astype(F32)
        keep_mine = 1.0 - even * second
        keep_theirs = 1.0 - (1.0 - even) * second
        merged[0] = (mine * keep_mine + theirs * keep_theirs).astype(BF16)
        for step in range(1, chips):
            chip_copy(step).start()

    def relay_chips():
        for step in range(1, chips):
            chip_copy(step).wait()
            relay_copy(step).start()

    def assemble():
        for step in range(1, chips):
            relay_copy(step).wait()
        pivot_col = state["pivot_col"]
        top = jnp.zeros((block, width), F32)
        for step in range(chips):
            low = (((chip + chips - step) % chips) * 2 * rows).astype(F32)
            here = (pivot_col >= low) & (pivot_col < low + 2 * rows)
            top = top + jnp.where(here, merged[step].astype(F32), 0.0)
        state["top"] = top.astype(BF16)

        @pl.when(me_r == 1)
        def _():
            homes[:, :width] = picked_in[...]

        for step in range(1, chips):
            @pl.when((chip > 0) & (chip == step))
            def _():
                homes[:, :width] = merged[step]

    def interchange(start):
        def act():
            row = iota((block, block), 0) + (me_r * rows + start)
            pivot_row = state["pivot_row"]
            hot = jnp.where((row.astype(F32) == pivot_row) & (pivot_row >= block), 1.0, 0.0)
            both = dot(hot.astype(BF16), homes[...])
            taken = both[:, width:] > 0.5
            for lane in range(0, width, LANES):
                kept = slab_ref[start:start + block, lane:lane + LANES].astype(F32)
                new = jnp.where(taken, both[:, lane:lane + LANES], kept)
                pivoted[start:start + block, lane:lane + LANES] = new.astype(BF16)
        return act

    base = min(block, 256)
    small = min(base, 16)
    bi = iota((base, base), 0)
    bj = iota((base, base), 1)
    groups = block // base

    def diagonal(g):
        part = l_top_ref[g * base:(g + 1) * base, g * base:(g + 1) * base].astype(F32)
        return jnp.where(bi > bj, part, 0.0)

    def start_inverse():
        l_top_copy.wait()
        state["x"], state["power"] = [], []
        for g in range(groups):
            near = jnp.where(bi // small == bj // small, diagonal(g), 0.0)
            state["x"].append(jnp.where(bi == bj, 1.0, 0.0) - near)
            exact = near.astype(BF16)
            state["power"].append(dot(exact, exact))

    def power_step():
        for g in range(groups):
            x, power = state["x"][g], state["power"][g]
            state["x"][g] = x + dot_split(x, power)
            state["power"][g] = dot_split(power, power)

    def last_power():
        for g in range(groups):
            x, power = state["x"][g], state["power"][g]
            state["x"][g] = x + dot_split(x, power)

    def double(size):
        def act():
            for g in range(groups):
                link = jnp.where(
                    (bi // (2 * size) == bj // (2 * size)) & (bi // size != bj // size), diagonal(g), 0.0
                )
                inv = state["x"][g]
                state["x"][g] = inv - dot_split(inv, dot_exact_left(link.astype(BF16), inv))
        return act

    def join():
        for g in range(groups):
            high[g * base:(g + 1) * base, :] = jnp.zeros((base, block), F32)
            high[g * base:(g + 1) * base, g * base:(g + 1) * base] = state["x"][g]

    def join_double(size):
        def act():
            for at in range(0, block, 2 * size):
                a = high[at:at + size, at:at + size]
                b = high[at + size:at + 2 * size, at + size:at + 2 * size]
                c = l_top_ref[at + size:at + 2 * size, at:at + size]
                high[at + size:at + 2 * size, at:at + size] = -dot_split(b, dot_exact_left(c, a))
        return act

    def split():
        inverse_hi[...], inverse_lo[...] = halves(high[...])

    def solve():
        top = state["top"]
        u_ref[...] = (dot(inverse_hi[...], top) + dot(inverse_lo[...], top)).astype(BF16)

    inverse = [start_inverse]
    size = 4
    while size < small:
        inverse.append(power_step)
        size *= 2
    if small > 2:
        inverse.append(last_power)
    size = small
    while size < base:
        inverse.append(double(size))
        size *= 2
    inverse.append(join)
    while size < block:
        inverse.append(join_double(size))
        size *= 2
    inverse.append(split)

    def update(piece):
        start, size = pieces[piece]

        def act():
            panel = gathered[:, :, start:start + size].reshape(block, size).astype(BF16)
            out_ref[start:start + size, :] = trailing(panel, u_ref[...], pivoted[start:start + size, :])

        needed(piece, act)
        if start < block:
            @pl.when(lead)
            def _():
                end = min(block, start + size)
                out_ref[start:end, :] = u_ref[start:end, :]

    pl.semaphore_wait(barrier, 1 + chips + has_below + has_above)
    panel_copy.wait()
    first_sends()
    bookkeeping()
    pick()
    core_copy().start()

    own_homes()

    def relays(distance):
        return [relay(distance, piece) for piece in bulk] if distance < length else []

    changes = [interchange(start) for start in range(0, rows, block)]
    plan = inverse[:3] + [merge] + weave(relays(1), inverse[3:6])
    plan += [other_rest, own_rest(0, other), own_rest(1, x), own_rest(1, other)] + inverse[6:8]
    second = relays(2)
    half_way = len(second) // 2
    plan += weave(second[:half_way], inverse[8:10]) + [pass_rest(1, 1)]
    plan += weave(second[half_way:], [relay_chips] + inverse[10:])
    plan += [own_rest(2, x), own_rest(2, other), pass_rest(2, 1), assemble, solve]
    plan += weave(relays(3), changes[:3] + [pass_rest(2, 2)]) + changes[3:]
    for distance in range(3, length):
        plan += relays(distance) if distance > 3 else []
        plan += [own_rest(distance, x), own_rest(distance, other)]
        plan += [pass_rest(distance, reach) for reach in range(1, distance + 1)]
    for act in plan:
        act()

    late = late_pieces(block, rows)
    for piece in bulk:
        crossed(piece)
        if piece not in late:
            update(piece)
    last_rests()
    if rest not in late:
        update(rest)

    drain()


def finish(done_ref, gathered, pivoted, u_ref, out_hbm, result, sem):
    block = u_ref.shape[0]
    pieces = cuts(gathered.shape[2])
    late = late_pieces(block, gathered.shape[2])
    early = pieces[late[0]][0] if late else gathered.shape[2]
    copies = []

    def store(source, first, size):
        copy = pltpu.make_async_copy(source.at[pl.ds(first, size)], out_hbm.at[pl.ds(first, size)], sem.at[len(copies)])
        copy.start()
        copies.append(copy)

    store(done_ref, 0, early)
    for piece in late:
        start, size = pieces[piece]
        panel = gathered[:, :, start:start + size].reshape(block, size).astype(BF16)
        result[start:start + size, :] = trailing(panel, u_ref[...], pivoted[start:start + size, :])
        store(result, start, size)
    for copy in copies:
        copy.wait()


def per_device(n_prow, n_pcol, slab, pivots, l_top, l_panel_t):
    rows, width = slab.shape
    block = pivots.shape[0]
    depth = l_panel_t.shape[0]
    kind = BF16 if depth % 16 == 0 else F32
    panel = l_panel_t.astype(kind)
    chips = n_prow // 2
    n_pieces = len(cuts(rows))
    vmem = pl.BlockSpec(memory_space=pltpu.VMEM)
    anywhere = pl.BlockSpec(memory_space=pltpu.HBM)
    dma = pltpu.SemaphoreType.DMA
    kept = [
        pltpu.VMEM((rows, width), BF16),
        pltpu.VMEM((n_pcol, depth, rows), kind),
        pltpu.VMEM((rows, width), BF16),
        pltpu.VMEM((block, width), BF16),
    ]
    done, gathered, pivoted, u = pl.pallas_call(
        functools.partial(kernel, n_prow, n_pcol),
        out_shape=kept,
        in_specs=[anywhere] * 4,
        out_specs=[vmem] * 4,
        scratch_shapes=[
            pltpu.VMEM((rows, width), BF16),
            pltpu.VMEM((1, block), jnp.int32),
            pltpu.VMEM((block, block), BF16),
            pltpu.VMEM((block, width), BF16),
            pltpu.VMEM((block, width), BF16),
            pltpu.VMEM((chips, block, width), BF16),
            pltpu.VMEM((block, width + LANES), BF16),
            pltpu.VMEM((block, block), BF16),
            pltpu.VMEM((block, block), BF16),
            pltpu.VMEM((block, block), F32),
            dma((4,)),
            dma((n_pcol // 2, n_pieces - 1)),
            dma((n_pieces - 1,)),
            dma((n_pcol // 2, 2)),
            dma((6,)),
            dma((2,)),
            dma((chips - 1,)),
            dma((chips - 1,)),
            dma((chips - 1,)),
            dma((chips - 1,)),
        ],
        compiler_params=pltpu.CompilerParams(collective_id=0, has_side_effects=True, vmem_limit_bytes=LIMIT),
    )(slab, pivots.reshape(1, block), l_top, panel)
    return pl.pallas_call(
        finish,
        out_shape=pltpu.HBM((rows, width), BF16),
        in_specs=[vmem] * 4,
        out_specs=anywhere,
        scratch_shapes=[pltpu.VMEM((rows, width), BF16), dma((n_pieces,))],
        compiler_params=pltpu.CompilerParams(vmem_limit_bytes=16 * 2**20),
    )(done, gathered, pivoted, u)


def solution(mesh):
    return jax.shard_map(
        functools.partial(per_device, mesh.shape["prow"], mesh.shape["pcol"]),
        mesh=mesh,
        in_specs=(P("prow", "pcol"), P(), P(), P("pcol", "prow")),
        out_specs=P("prow", "pcol"),
        check_vma=False,
    )
```

```python
import functools

import jax
import jax.numpy as jnp
from jax import lax
from jax.experimental import pallas as pl
from jax.experimental.pallas import tpu as pltpu
from jax.sharding import PartitionSpec as P

MESH = pl.DeviceIdType.MESH
F32 = jnp.float32
BF16 = jnp.bfloat16
LANES = 128


def dot(a, b):
    return jnp.dot(a, b, preferred_element_type=F32)


def iota(shape, axis):
    return lax.broadcasted_iota(jnp.int32, shape, axis)


def halves(a):
    high = a.astype(BF16)
    return high, (a - high.astype(F32)).astype(BF16)


def dot_exact_left(a, b):
    high, low = halves(b)
    return dot(a, high) + dot(a, low)


def dot_split(a, b):
    a_high, a_low = halves(a)
    b_high, b_low = halves(b)
    return dot(a_high, b_high) + (dot(a_high, b_low) + dot(a_low, b_high))


STRIPS = (0, 4, 7, 10)
THICK = 12
THIN = 14
LIMIT = 54 * 2**20


def cuts(width, thick=True):
    units = width // LANES
    edges = [units * part // 16 * LANES for part in STRIPS + (THICK if thick else THIN, 16)]
    return [(a, b - a) for a, b in zip(edges[:-1], edges[1:])]


def box(columns, shape):
    for count in range(1, shape[0] + 1):
        if columns % (count * LANES) == 0 and columns // count <= shape[2]:
            return count, columns // count


def level_of(gathered, u_ref, level, columns):
    depth = 2 * gathered.shape[1]
    panel = gathered[pl.ds(level * 2, 2), :, columns[0]:columns[0] + columns[1]].reshape(depth, columns[1])
    return lax.dot_general(
        panel.astype(BF16), u_ref[pl.ds(pl.multiple_of(level * depth, depth), depth), :],
        (((0,), (0,)), ((), ())), preferred_element_type=F32,
    )


def last_level(length):
    z = lax.axis_index("pcol") // 2
    return jnp.where(z < length // 2, length - 1, 0)


def weave(events, work):
    plan, count = [], max(1, len(events))
    for at, event in enumerate(events):
        plan += [event] + work[at * len(work) // count:(at + 1) * len(work) // count]
    return plan


def trailing(panel, u, rows):
    product = lax.dot_general(panel, u, (((0,), (0,)), ((), ())), preferred_element_type=F32)
    return (rows.astype(F32) - product).astype(BF16)


def kernel(
    n_prow, n_pcol,
    slab_hbm, pivots_hbm, l_top_hbm, panel_hbm, out_ref, gathered, u_ref, partial, pivoted,
    slab_ref, pivots_ref, l_top_ref, picked, picked_in, merged, homes, inverse_hi, inverse_lo, high,
    local_sem, line_recv, cross_recv, rest_recv, sent, core_sem, chip_send, chip_recv, relay_send, relay_recv,
):
    block = l_top_ref.shape[0]
    rows, width = slab_ref.shape
    me_r = lax.axis_index("prow")
    me_c = lax.axis_index("pcol")
    chips = n_prow // 2
    chip, core = me_r // 2, me_r % 2
    peer = me_r + 1 - 2 * core
    length = n_pcol // 2
    z, x = me_c // 2, me_c % 2
    other = 1 - x
    pieces = cuts(gathered.shape[2])
    bulk = range(len(pieces) - 1)
    rest = len(pieces) - 1
    lead = me_r == 0

    def needed(piece, act):
        start, size = pieces[piece]
        if start + size <= block:
            pl.when(jnp.logical_not(lead))(act)
        else:
            act()

    panel_copy = pltpu.make_async_copy(panel_hbm, gathered.at[me_c], local_sem.at[0])
    pivots_copy = pltpu.make_async_copy(pivots_hbm, pivots_ref, local_sem.at[1])
    slab_copy = pltpu.make_async_copy(slab_hbm, slab_ref, local_sem.at[2])
    l_top_copy = pltpu.make_async_copy(l_top_hbm, l_top_ref, local_sem.at[3])

    barrier = pltpu.get_barrier_semaphore()

    def greet(r, c):
        pl.semaphore_signal(barrier, inc=1, device_id=(r, c), device_id_type=MESH)

    greet(me_r, z * 2 + other)

    @pl.when(z > 0)
    def _():
        greet(me_r, me_c - 2)

    @pl.when(z < length - 1)
    def _():
        greet(me_r, me_c + 2)

    for step in range(1, chips):
        greet(((chip + step) % chips) * 2 + core, me_c)
    greet(peer, me_c)

    panel_copy.start()
    pivots_copy.start()
    slab_copy.start()
    l_top_copy.start()

    has_below = (z + length - 1) // length
    has_above = (2 * length - 2 - z) // length

    tail = rest - 1
    mixed = length == 4

    def by_class(at, act):
        if mixed:
            outer = ((at == 0) | (at == length - 1)) & jnp.logical_not(lead)
            pl.when(outer)(lambda: act(True))
            pl.when(jnp.logical_not(outer))(lambda: act(False))
        else:
            act(True)

    def columns_of(piece, thick):
        return cuts(gathered.shape[2], thick)[piece]

    def send(source, columns, send_sem, recv_sem, target):
        part = gathered.at[source, :, pl.ds(*columns)]
        pltpu.make_async_remote_copy(
            src_ref=part, dst_ref=part, send_sem=send_sem, recv_sem=recv_sem,
            device_id=(me_r, target), device_id_type=MESH,
        ).start()

    def arrival(columns, send_sem, recv_sem):
        count, size = box(columns, gathered.shape)
        part = gathered.at[pl.ds(0, count), :, pl.ds(0, size)]
        return pltpu.make_async_remote_copy(
            src_ref=part, dst_ref=part, send_sem=send_sem, recv_sem=recv_sem,
            device_id=(me_r, z * 2 + other), device_id_type=MESH,
        )

    def landed(columns, recv_sem):
        arrival(columns, sent.at[0], recv_sem).wait_recv()

    def neighbour(way):
        return me_c + 2 - 4 * way

    def line(way, at, piece, thick):
        send(at * 2 + x, columns_of(piece, thick), sent.at[way], line_recv.at[at, piece], neighbour(way))

    def cross(at, piece, thick):
        send(at * 2 + x, columns_of(piece, thick), sent.at[4], cross_recv.at[piece], z * 2 + other)

    def line_rest(way, at, side, thick):
        send(at * 2 + side, columns_of(rest, thick), sent.at[2 + way], rest_recv.at[at], neighbour(way))

    def classed(at, piece, act):
        if piece >= tail:
            by_class(at, act)
        else:
            act(True)

    def both_ways(act):
        pl.when(z < length - 1)(lambda: act(0))
        pl.when(z > 0)(lambda: act(1))

    def first_sends():
        for piece in bulk:
            def own(thick):
                both_ways(lambda way: line(way, z, piece, thick))
                cross(z, piece, thick)
            needed(piece, lambda: classed(z, piece, own))
            if piece == 0:
                by_class(z, lambda thick: send(
                    me_c, columns_of(rest, thick), sent.at[5], rest_recv.at[z], z * 2 + other
                ))
        own_rest(0, x)()

    def rest_ways(distance, act):
        if distance < length - 1:
            pl.when(z == distance)(lambda: act(0))
            pl.when(z == length - 1 - distance)(lambda: act(1))

    def own_rest(distance, side):
        def act(way):
            by_class(z, lambda thick: line_rest(way, z, side, thick))
        return lambda: rest_ways(distance, act)

    def other_rest():
        by_class(z, lambda thick: landed(columns_of(rest, thick)[1], rest_recv.at[z]))

    def both_rests(at, act=None):
        def classed_act(thick):
            landed(2 * columns_of(rest, thick)[1], rest_recv.at[at])
            if act is not None:
                for side in (0, 1):
                    act(side, thick)
        by_class(at, classed_act)

    def pass_rest(distance, reach):
        def onward(way):
            at = z + (2 * way - 1) * reach
            both_rests(at, lambda side, thick: line_rest(way, at, side, thick))
        return lambda: rest_ways(distance, onward)

    def relay(distance, piece):
        def both():
            for way, at, reached, onward in (
                (0, z - distance, z >= distance, z < length - 1),
                (1, z + distance, z < length - distance, z > 0),
            ):
                def pass_on(thick):
                    landed(columns_of(piece, thick)[1], line_recv.at[at, piece])
                    pl.when(onward)(lambda: line(way, at, piece, thick))
                    cross(at, piece, thick)

                pl.when(reached)(lambda: classed(at, piece, pass_on))
        return lambda: needed(piece, both)

    def last_rests(distance):
        for way, at, reached in (
            (0, z - distance, (z >= distance) & (z == length - 1)),
            (1, z + distance, (z < length - distance) & (z == 0)),
        ):
            pl.when(reached)(lambda: both_rests(at))

    def lanes_of(pieces_of, levels, leading):
        total = 0
        for at in levels:
            thick = not mixed or (not leading and at in (0, length - 1))
            for piece in pieces_of:
                start, size = columns_of(piece, thick)
                total += 0 if leading and start + size <= block else size
        return total

    def for_lead(act):
        pl.when(lead)(lambda: act(True))
        pl.when(jnp.logical_not(lead))(lambda: act(False))

    def crossed(piece):
        if piece == tail:
            for_lead(lambda leading: landed(lanes_of([tail], range(length), leading), cross_recv.at[tail]))
        else:
            needed(piece, lambda: landed(length * pieces[piece][1], cross_recv.at[piece]))

    def drain():
        def gone(sem, columns):
            arrival(columns, sent.at[sem], rest_recv.at[0]).wait_send()

        def act(leading):
            for at in range(length):
                def here():
                    if at < length - 1:
                        gone(0, lanes_of(bulk, range(at + 1), leading))
                        gone(2, 2 * lanes_of([rest], range(at + 1), leading))
                    if at > 0:
                        gone(1, lanes_of(bulk, range(at, length), leading))
                        gone(3, 2 * lanes_of([rest], range(at, length), leading))
                    gone(5, lanes_of([rest], [at], leading))
                pl.when(z == at)(here)
            gone(4, lanes_of(bulk, range(length), leading))

        for_lead(act)

    state = {}
    ii = iota((block, block), 0)
    jj = iota((block, block), 1)

    def column(row):
        return jnp.sum(jnp.where(ii == jj, row, 0.0), axis=1, keepdims=True)

    def bookkeeping():
        pivots_copy.wait()
        pivot_row = pivots_ref[...].astype(F32)
        pivot_col = column(pivot_row)
        chosen = jnp.max(jnp.where(pivot_col == jj.astype(F32), 1.0, 0.0), axis=0, keepdims=True)
        free = 1.0 - chosen
        far = jnp.where(pivot_row >= block, 1.0, 0.0)
        which = iota((16, block), 0)
        both = jnp.where(which == 0, free, jnp.where(which == 1, far, 0.0))
        ranks = dot(both.astype(BF16), jnp.where(ii < jj, 1.0, 0.0).astype(BF16))
        far_rank = column(ranks[1:2])
        match = (free > 0.5) & (ranks[0:1] == far_rank)
        source = jnp.sum(jnp.where(match, jj.astype(F32), 0.0), axis=1, keepdims=True)
        state.update(pivot_row=pivot_row, pivot_col=pivot_col, source=source)

    def pick():
        pivot_col, source = state["pivot_col"], state["source"]
        first = (me_r * rows).astype(F32)
        mine = (pivot_col >= first) & (pivot_col < first + rows)
        holds = lead.astype(F32)
        index = jnp.where(mine, pivot_col - first, source * holds - (1.0 - holds))
        slab_copy.wait()
        total = jnp.zeros((block, width), F32)
        for start in range(0, rows, block):
            hot = jnp.where((jj + start).astype(F32) == index, 1.0, 0.0).astype(BF16)
            total = total + dot(hot, slab_ref[start:start + block, :])
        picked[...] = total.astype(BF16)

    def core_copy():
        return pltpu.make_async_remote_copy(
            src_ref=picked, dst_ref=picked_in, send_sem=core_sem.at[0], recv_sem=core_sem.at[1],
            device_id=(peer, me_c), device_id_type=MESH,
        )

    def own_homes():
        homes[:, width:] = jnp.ones((block, LANES), BF16)

        @pl.when(me_r == 0)
        def _():
            hot = jnp.where(jj.astype(F32) == state["source"], 1.0, 0.0).astype(BF16)
            homes[:, :width] = dot(hot, slab_ref[:block, :]).astype(BF16)

    half = block // 2

    def chip_copy(step):
        rows_of = pl.ds(pl.multiple_of(core * half, half), half)
        to = ((chip + step) % chips) * 2 + core
        return pltpu.make_async_remote_copy(
            src_ref=merged.at[0, rows_of], dst_ref=merged.at[step, rows_of],
            send_sem=chip_send.at[step - 1], recv_sem=chip_recv.at[step - 1],
            device_id=(to, me_c), device_id_type=MESH,
        )

    def relay_copy(step):
        part = merged.at[step, pl.ds(pl.multiple_of(core * half, half), half)]
        return pltpu.make_async_remote_copy(
            src_ref=part, dst_ref=part, send_sem=relay_send.at[step - 1], recv_sem=relay_recv.at[step - 1],
            device_id=(peer, me_c), device_id_type=MESH,
        )

    def merge():
        core_copy().wait()
        pivot_col = state["pivot_col"]
        holds = (chip == 0).astype(F32)
        second = jnp.where((pivot_col >= rows) & (pivot_col < 2 * rows), holds, 0.0)
        mine, theirs = picked[...].astype(F32), picked_in[...].astype(F32)
        even = (core == 0).astype(F32)
        keep_mine = 1.0 - even * second
        keep_theirs = 1.0 - (1.0 - even) * second
        merged[0] = (mine * keep_mine + theirs * keep_theirs).astype(BF16)
        for step in range(1, chips):
            chip_copy(step).start()

    def relay_chips():
        for step in range(1, chips):
            chip_copy(step).wait()
            relay_copy(step).start()

    def assemble():
        for step in range(1, chips):
            relay_copy(step).wait()
        pivot_col = state["pivot_col"]
        top = jnp.zeros((block, width), F32)
        for step in range(chips):
            low = (((chip + chips - step) % chips) * 2 * rows).astype(F32)
            here = (pivot_col >= low) & (pivot_col < low + 2 * rows)
            top = top + jnp.where(here, merged[step].astype(F32), 0.0)
        state["top"] = top.astype(BF16)

        @pl.when(me_r == 1)
        def _():
            homes[:, :width] = picked_in[...]

        for step in range(1, chips):
            @pl.when((chip > 0) & (chip == step))
            def _():
                homes[:, :width] = merged[step]

    def interchange(start):
        def act():
            row = iota((block, block), 0) + (me_r * rows + start)
            pivot_row = state["pivot_row"]
            hot = jnp.where((row.astype(F32) == pivot_row) & (pivot_row >= block), 1.0, 0.0)
            both = dot(hot.astype(BF16), homes[...])
            taken = both[:, width:] > 0.5
            for lane in range(0, width, LANES):
                kept = slab_ref[start:start + block, lane:lane + LANES].astype(F32)
                new = jnp.where(taken, both[:, lane:lane + LANES], kept)
                pivoted[start:start + block, lane:lane + LANES] = new.astype(BF16)
        return act

    base = min(block, 256)
    small = min(base, 16)
    bi = iota((base, base), 0)
    bj = iota((base, base), 1)
    groups = block // base

    def diagonal(g):
        part = l_top_ref[g * base:(g + 1) * base, g * base:(g + 1) * base].astype(F32)
        return jnp.where(bi > bj, part, 0.0)

    def start_inverse():
        l_top_copy.wait()
        state["x"], state["power"] = [], []
        for g in range(groups):
            near = jnp.where(bi // small == bj // small, diagonal(g), 0.0)
            state["x"].append(jnp.where(bi == bj, 1.0, 0.0) - near)
            exact = near.astype(BF16)
            state["power"].append(dot(exact, exact))

    def power_step():
        for g in range(groups):
            x, power = state["x"][g], state["power"][g]
            state["x"][g] = x + dot_split(x, power)
            state["power"][g] = dot_split(power, power)

    def last_power():
        for g in range(groups):
            x, power = state["x"][g], state["power"][g]
            state["x"][g] = x + dot_split(x, power)

    def double(size):
        def act():
            for g in range(groups):
                link = jnp.where(
                    (bi // (2 * size) == bj // (2 * size)) & (bi // size != bj // size), diagonal(g), 0.0
                )
                inv = state["x"][g]
                state["x"][g] = inv - dot_split(inv, dot_exact_left(link.astype(BF16), inv))
        return act

    def join():
        for g in range(groups):
            high[g * base:(g + 1) * base, :] = jnp.zeros((base, block), F32)
            high[g * base:(g + 1) * base, g * base:(g + 1) * base] = state["x"][g]

    def join_double(size):
        def act():
            for at in range(0, block, 2 * size):
                a = high[at:at + size, at:at + size]
                b = high[at + size:at + 2 * size, at + size:at + 2 * size]
                c = l_top_ref[at + size:at + 2 * size, at:at + size]
                high[at + size:at + 2 * size, at:at + size] = -dot_split(b, dot_exact_left(c, a))
        return act

    def split():
        inverse_hi[...], inverse_lo[...] = halves(high[...])

    def solve():
        top = state["top"]
        u_ref[...] = (dot(inverse_hi[...], top) + dot(inverse_lo[...], top)).astype(BF16)

    inverse = [start_inverse]
    size = 4
    while size < small:
        inverse.append(power_step)
        size *= 2
    if small > 2:
        inverse.append(last_power)
    size = small
    while size < base:
        inverse.append(double(size))
        size *= 2
    inverse.append(join)
    while size < block:
        inverse.append(join_double(size))
        size *= 2
    inverse.append(split)

    def update(piece):
        start, size = pieces[piece]

        def act():
            panel = gathered[:, :, start:start + size].reshape(block, size).astype(BF16)
            out_ref[start:start + size, :] = trailing(panel, u_ref[...], pivoted[start:start + size, :])

        needed(piece, act)
        if start < block:
            @pl.when(lead)
            def _():
                end = min(block, start + size)
                out_ref[start:end, :] = u_ref[start:end, :]

    pl.semaphore_wait(barrier, 1 + chips + has_below + has_above)
    panel_copy.wait()
    first_sends()
    bookkeeping()
    pick()
    core_copy().start()

    own_homes()

    def relays(distance):
        return [relay(distance, piece) for piece in bulk] if distance < length else []

    changes = [interchange(start) for start in range(0, rows, block)]
    plan = inverse[:3] + [merge] + weave(relays(1), inverse[3:6])
    plan += [other_rest, own_rest(0, other), own_rest(1, x), own_rest(1, other)] + inverse[6:8]
    second = relays(2)
    half_way = len(second) // 2
    plan += weave(second[:half_way], inverse[8:10]) + [pass_rest(1, 1)]
    plan += weave(second[half_way:], [relay_chips] + inverse[10:])
    plan += [own_rest(2, x), own_rest(2, other), pass_rest(2, 1), assemble, solve]
    plan += weave(relays(3), changes[:3] + [pass_rest(2, 2)]) + changes[3:]
    for distance in range(3, length):
        plan += relays(distance) if distance > 3 else []
        plan += [own_rest(distance, x), own_rest(distance, other)]
        plan += [pass_rest(distance, reach) for reach in range(1, distance + 1)]
    for act in plan:
        act()

    for piece in bulk:
        if piece == 0:
            for distance in range(1, length - 1):
                last_rests(distance)
            start, size = columns_of(rest, False)
            total = pivoted[start:start + size, :].astype(F32)
            last = last_level(length)
            for step in range(1, length):
                total = total - level_of(gathered, u_ref, (last + step) % length, (start, size))
            partial[...] = total
        crossed(piece)
        if piece < tail:
            update(piece)
    last_rests(length - 1)

    drain()


def finish(done_ref, gathered, u_ref, partial, pivoted, out_hbm, result, sem):
    block = u_ref.shape[0]
    edge = cuts(gathered.shape[2])[-2][0]
    start, size = cuts(gathered.shape[2], False)[-1]

    def store(source, start, size, n):
        copy = pltpu.make_async_copy(source, out_hbm.at[pl.ds(start, size)], sem.at[n])
        copy.start()
        return copy

    copies = [store(done_ref.at[pl.ds(0, edge)], 0, edge, 0)]
    panel = gathered[:, :, edge:start].reshape(block, start - edge).astype(BF16)
    result[:start - edge, :] = trailing(panel, u_ref[...], pivoted[edge:start, :])
    copies.append(store(result.at[pl.ds(0, start - edge)], edge, start - edge, 2))
    last = last_level(gathered.shape[0] // 2)
    result[start - edge:, :] = (partial[...] - level_of(gathered, u_ref, last, (start, size))).astype(BF16)
    copies.append(store(result.at[pl.ds(start - edge, size)], start, size, 1))
    for copy in copies:
        copy.wait()


def per_device(n_prow, n_pcol, slab, pivots, l_top, l_panel_t):
    rows, width = slab.shape
    block = pivots.shape[0]
    depth = l_panel_t.shape[0]
    kind = BF16 if depth % 16 == 0 else F32
    panel = l_panel_t.astype(kind)
    chips = n_prow // 2
    n_pieces = len(cuts(rows))
    vmem = pl.BlockSpec(memory_space=pltpu.VMEM)
    anywhere = pl.BlockSpec(memory_space=pltpu.HBM)
    dma = pltpu.SemaphoreType.DMA
    kept = [
        pltpu.VMEM((rows, width), BF16),
        pltpu.VMEM((n_pcol, depth, rows), kind),
        pltpu.VMEM((block, width), BF16),
        pltpu.VMEM((cuts(rows, False)[-1][1], width), F32),
        pltpu.VMEM((rows, width), BF16),
    ]
    done, gathered, u, partial, pivoted = pl.pallas_call(
        functools.partial(kernel, n_prow, n_pcol),
        out_shape=kept,
        in_specs=[anywhere] * 4,
        out_specs=[vmem] * 5,
        scratch_shapes=[
            pltpu.VMEM((rows, width), BF16),
            pltpu.VMEM((1, block), jnp.int32),
            pltpu.VMEM((block, block), BF16),
            pltpu.VMEM((block, width), BF16),
            pltpu.VMEM((block, width), BF16),
            pltpu.VMEM((chips, block, width), BF16),
            pltpu.VMEM((block, width + LANES), BF16),
            pltpu.VMEM((block, block), BF16),
            pltpu.VMEM((block, block), BF16),
            pltpu.VMEM((block, block), F32),
            dma((4,)),
            dma((n_pcol // 2, n_pieces - 1)),
            dma((n_pieces - 1,)),
            dma((n_pcol // 2,)),
            dma((6,)),
            dma((2,)),
            dma((chips - 1,)),
            dma((chips - 1,)),
            dma((chips - 1,)),
            dma((chips - 1,)),
        ],
        compiler_params=pltpu.CompilerParams(collective_id=0, has_side_effects=True, vmem_limit_bytes=LIMIT),
    )(slab, pivots.reshape(1, block), l_top, panel)
    return pl.pallas_call(
        finish,
        out_shape=pltpu.HBM((rows, width), BF16),
        in_specs=[vmem] * 5,
        out_specs=anywhere,
        scratch_shapes=[pltpu.VMEM((rows - cuts(rows)[-2][0], width), BF16), dma((3,))],
        compiler_params=pltpu.CompilerParams(vmem_limit_bytes=16 * 2**20),
    )(done, gathered, u, partial, pivoted)


def solution(mesh):
    return jax.shard_map(
        functools.partial(per_device, mesh.shape["prow"], mesh.shape["pcol"]),
        mesh=mesh,
        in_specs=(P("prow", "pcol"), P(), P(), P("pcol", "prow")),
        out_specs=P("prow", "pcol"),
        check_vma=False,
    )
```

```python
import functools

import jax
import jax.numpy as jnp
from jax import lax
from jax.experimental import pallas as pl
from jax.experimental.pallas import tpu as pltpu
from jax.sharding import PartitionSpec as P

MESH = pl.DeviceIdType.MESH
F32 = jnp.float32
BF16 = jnp.bfloat16
LANES = 128


def dot(a, b):
    return jnp.dot(a, b, preferred_element_type=F32)


def iota(shape, axis):
    return lax.broadcasted_iota(jnp.int32, shape, axis)


def halves(a):
    high = a.astype(BF16)
    return high, (a - high.astype(F32)).astype(BF16)


def dot_exact_left(a, b):
    high, low = halves(b)
    return dot(a, high) + dot(a, low)


def dot_split(a, b):
    a_high, a_low = halves(a)
    b_high, b_low = halves(b)
    return dot(a_high, b_high) + (dot(a_high, b_low) + dot(a_low, b_high))


STRIPS = (0, 4, 7, 10)
THICK = 12
THIN = 14
LIMIT = 54 * 2**20


def cuts(width, thick=True):
    units = width // LANES
    edges = [units * part // 16 * LANES for part in STRIPS + (THICK if thick else THIN, 16)]
    return [(a, b - a) for a, b in zip(edges[:-1], edges[1:])]


def box(columns, shape):
    for count in range(1, shape[0] + 1):
        if columns % (count * LANES) == 0 and columns // count <= shape[2]:
            return count, columns // count


def level_of(gathered, u_ref, level, columns):
    depth = 2 * gathered.shape[1]
    panel = gathered[pl.ds(level * 2, 2), :, columns[0]:columns[0] + columns[1]].reshape(depth, columns[1])
    return lax.dot_general(
        panel.astype(BF16), u_ref[pl.ds(pl.multiple_of(level * depth, depth), depth), :],
        (((0,), (0,)), ((), ())), preferred_element_type=F32,
    )


def last_level(length):
    z = lax.axis_index("pcol") // 2
    return jnp.where(z < length // 2, length - 1, 0)


def weave(events, work):
    plan, count = [], max(1, len(events))
    for at, event in enumerate(events):
        plan += [event] + work[at * len(work) // count:(at + 1) * len(work) // count]
    return plan


def trailing(panel, u, rows):
    product = lax.dot_general(panel, u, (((0,), (0,)), ((), ())), preferred_element_type=F32)
    return (rows.astype(F32) - product).astype(BF16)


def kernel(
    n_prow, n_pcol,
    slab_hbm, pivots_hbm, l_top_hbm, panel_hbm, out_ref, gathered, u_ref, partial, pivoted,
    slab_ref, pivots_ref, l_top_ref, picked, picked_in, merged, homes, inverse_hi, inverse_lo, high, guest,
    local_sem, line_recv, cross_recv, rest_recv, sent, guest_sem, ready, core_sem, chip_send, chip_recv, relay_send, relay_recv,
):
    block = l_top_ref.shape[0]
    rows, width = slab_ref.shape
    me_r = lax.axis_index("prow")
    me_c = lax.axis_index("pcol")
    chips = n_prow // 2
    chip, core = me_r // 2, me_r % 2
    peer = me_r + 1 - 2 * core
    length = n_pcol // 2
    z, x = me_c // 2, me_c % 2
    other = 1 - x
    pieces = cuts(gathered.shape[2])
    bulk = range(len(pieces) - 1)
    rest = len(pieces) - 1
    lead = me_r == 0

    def needed(piece, act):
        start, size = pieces[piece]
        if start + size <= block:
            pl.when(jnp.logical_not(lead))(act)
        else:
            act()

    panel_copy = pltpu.make_async_copy(panel_hbm, gathered.at[me_c], local_sem.at[0])
    pivots_copy = pltpu.make_async_copy(pivots_hbm, pivots_ref, local_sem.at[1])
    slab_copy = pltpu.make_async_copy(slab_hbm, slab_ref, local_sem.at[2])
    l_top_copy = pltpu.make_async_copy(l_top_hbm, l_top_ref, local_sem.at[3])

    barrier = pltpu.get_barrier_semaphore()

    def greet(r, c):
        pl.semaphore_signal(barrier, inc=1, device_id=(r, c), device_id_type=MESH)

    greet(me_r, z * 2 + other)

    @pl.when(z > 0)
    def _():
        greet(me_r, me_c - 2)

    @pl.when(z < length - 1)
    def _():
        greet(me_r, me_c + 2)

    for step in range(1, chips):
        greet(((chip + step) % chips) * 2 + core, me_c)
    greet(peer, me_c)

    panel_copy.start()
    pivots_copy.start()
    slab_copy.start()
    l_top_copy.start()

    has_below = (z + length - 1) // length
    has_above = (2 * length - 2 - z) // length

    tail = rest - 1
    mixed = length == 4
    moves = n_prow == 4 and length <= 4
    giver = me_r == 2

    def by_class(at, act):
        if mixed:
            outer = ((at == 0) | (at == length - 1)) & jnp.logical_not(lead)
            pl.when(outer)(lambda: act(True))
            pl.when(jnp.logical_not(outer))(lambda: act(False))
        else:
            act(True)

    def columns_of(piece, kind):
        thick, given = kind if isinstance(kind, tuple) else (kind, False)
        start, size = cuts(gathered.shape[2], thick)[piece]
        return (start + LANES, size - LANES) if given and piece == tail else (start, size)

    def send(source, columns, send_sem, recv_sem, target):
        part = gathered.at[source, :, pl.ds(*columns)]
        pltpu.make_async_remote_copy(
            src_ref=part, dst_ref=part, send_sem=send_sem, recv_sem=recv_sem,
            device_id=(me_r, target), device_id_type=MESH,
        ).start()

    def arrival(columns, send_sem, recv_sem):
        count, size = box(columns, gathered.shape)
        part = gathered.at[pl.ds(0, count), :, pl.ds(0, size)]
        return pltpu.make_async_remote_copy(
            src_ref=part, dst_ref=part, send_sem=send_sem, recv_sem=recv_sem,
            device_id=(me_r, z * 2 + other), device_id_type=MESH,
        )

    def landed(columns, recv_sem):
        arrival(columns, sent.at[0], recv_sem).wait_recv()

    def neighbour(way):
        return me_c + 2 - 4 * way

    def line(way, at, piece, thick):
        send(at * 2 + x, columns_of(piece, thick), sent.at[way if piece < 2 else 2 + way], line_recv.at[at, piece], neighbour(way))

    def cross(at, piece, thick):
        send(at * 2 + x, columns_of(piece, thick), sent.at[4], cross_recv.at[piece], z * 2 + other)

    def line_rest(way, at, side, thick):
        send(at * 2 + side, columns_of(rest, thick), sent.at[2 + way], rest_recv.at[at], neighbour(way))

    def classed(at, piece, act):
        if piece == tail and moves:
            pl.when(giver)(lambda: by_class(at, lambda thick: act((thick, True))))
            pl.when(jnp.logical_not(giver))(lambda: by_class(at, act))
        elif piece >= tail:
            by_class(at, act)
        else:
            act(True)

    def both_ways(act):
        pl.when(z < length - 1)(lambda: act(0))
        pl.when(z > 0)(lambda: act(1))

    moved = pl.ds(pieces[tail][0], LANES)

    def guest_copy(source, target, recv_sem, row, column):
        return pltpu.make_async_remote_copy(
            src_ref=source, dst_ref=target, send_sem=guest_sem.at[4], recv_sem=recv_sem,
            device_id=(row, column), device_id_type=MESH,
        )

    def guest_total(count, recv_sem):
        rows_of, size = box(count * LANES, gathered.shape)
        part = gathered.at[pl.ds(0, rows_of), :, pl.ds(0, size)]
        return guest_copy(part, part, recv_sem, me_r, z * 2 + other)

    def only(who):
        return lambda act: pl.when(who)(act) if moves else None

    def guest_give():
        @only(giver)
        def _():
            guest_copy(gathered.at[me_c, :, moved], guest.at[me_c], guest_sem.at[0], 0, me_c).start()

    def guest_cross(source):
        part = guest.at[source]
        guest_copy(part, part, guest_sem.at[2], me_r, z * 2 + other).start()

    def guest_home(source):
        guest_copy(guest.at[source], gathered.at[source, :, moved], guest_sem.at[3], 2, me_c).start()

    def tell(n):
        @only(lead)
        def _():
            both_ways(lambda way: pl.semaphore_signal(
                ready.at[n], inc=1, device_id=(0, neighbour(way)), device_id_type=MESH
            ))

    def told(n):
        @only(lead)
        def _():
            pl.semaphore_wait(ready.at[n], has_below + has_above)

    def guest_own():
        told(1)

        @only(lead)
        def _():
            guest_total(1, guest_sem.at[0]).wait_recv()
            part = guest.at[me_c]
            for step in range(1, length):
                guest_copy(part, part, guest_sem.at[1], me_r, (z + step) % length * 2 + x).start()
            guest_cross(me_c)

    def guest_line():
        @only(lead)
        def _():
            guest_total(length - 1, guest_sem.at[1]).wait_recv()
            for step in range(1, length):
                guest_cross((z + step) % length * 2 + x)
            for step in range(1, length):
                guest_home((z + step) % length * 2 + x)

    def guest_other():
        @only(lead)
        def _():
            guest_total(length, guest_sem.at[2]).wait_recv()
            for at in range(length):
                guest_home(at * 2 + other)

    def guest_last():
        @only(giver)
        def _():
            guest_total(2 * length - 1, guest_sem.at[3]).wait_recv()

    def guest_drain():
        @only(giver)
        def _():
            guest_total(1, guest_sem.at[3]).wait_send()

        @only(lead)
        def _():
            guest_total(4 * length - 2, guest_sem.at[3]).wait_send()

    def first_sends():
        guest_give()
        for piece in bulk:
            def own(thick):
                both_ways(lambda way: line(way, z, piece, thick))
                cross(z, piece, thick)
            needed(piece, lambda: classed(z, piece, own))
            if piece == 0:
                by_class(z, lambda thick: send(
                    me_c, columns_of(rest, thick), sent.at[5], rest_recv.at[z], z * 2 + other
                ))
        own_rest(0, x)()

    def rest_ways(distance, act):
        if distance < length - 1:
            pl.when(z == distance)(lambda: act(0))
            pl.when(z == length - 1 - distance)(lambda: act(1))

    def own_rest(distance, side):
        def act(way):
            by_class(z, lambda thick: line_rest(way, z, side, thick))
        return lambda: rest_ways(distance, act)

    def other_rest():
        by_class(z, lambda thick: landed(columns_of(rest, thick)[1], rest_recv.at[z]))

    def both_rests(at, act=None):
        def classed_act(thick):
            landed(2 * columns_of(rest, thick)[1], rest_recv.at[at])
            if act is not None:
                for side in (0, 1):
                    act(side, thick)
        by_class(at, classed_act)

    def pass_rest(distance, reach):
        def onward(way):
            at = z + (2 * way - 1) * reach
            both_rests(at, lambda side, thick: line_rest(way, at, side, thick))
        return lambda: rest_ways(distance, onward)

    def relay(distance, piece):
        def both():
            for way, at, reached, onward in (
                (0, z - distance, z >= distance, z < length - 1),
                (1, z + distance, z < length - distance, z > 0),
            ):
                def pass_on(thick):
                    landed(columns_of(piece, thick)[1], line_recv.at[at, piece])
                    pl.when(onward)(lambda: line(way, at, piece, thick))
                    cross(at, piece, thick)

                pl.when(reached)(lambda: classed(at, piece, pass_on))
        return lambda: needed(piece, both)

    def last_rests(distance):
        for way, at, reached in (
            (0, z - distance, (z >= distance) & (z == length - 1)),
            (1, z + distance, (z < length - distance) & (z == 0)),
        ):
            pl.when(reached)(lambda: both_rests(at))

    def lanes_of(pieces_of, levels, kind):
        leading, given = kind
        total = 0
        for at in levels:
            thick = not mixed or (not leading and at in (0, length - 1))
            for piece in pieces_of:
                start, size = columns_of(piece, (thick, given))
                total += 0 if leading and start + size <= block else size
        return total

    def for_kinds(act):
        pl.when(lead)(lambda: act((True, False)))
        if moves:
            pl.when(giver)(lambda: act((False, True)))
            pl.when(jnp.logical_not(lead | giver))(lambda: act((False, False)))
        else:
            pl.when(jnp.logical_not(lead))(lambda: act((False, False)))

    def crossed(piece):
        if piece == tail:
            for_kinds(lambda kind: landed(lanes_of([tail], range(length), kind), cross_recv.at[tail]))
        else:
            needed(piece, lambda: landed(length * pieces[piece][1], cross_recv.at[piece]))

    def drain():
        def gone(sem, columns):
            arrival(columns, sent.at[sem], rest_recv.at[0]).wait_send()

        def act(kind):
            for at in range(length):
                def here():
                    if at < length - 1:
                        gone(0, lanes_of(range(2), range(at + 1), kind))
                        gone(2, lanes_of([*range(2, rest), rest, rest], range(at + 1), kind))
                    if at > 0:
                        gone(1, lanes_of(range(2), range(at, length), kind))
                        gone(3, lanes_of([*range(2, rest), rest, rest], range(at, length), kind))
                    gone(5, lanes_of([rest], [at], kind))
                pl.when(z == at)(here)
            gone(4, lanes_of(bulk, range(length), kind))

        for_kinds(act)
        guest_drain()

    state = {}
    ii = iota((block, block), 0)
    jj = iota((block, block), 1)

    def column(row):
        return jnp.sum(jnp.where(ii == jj, row, 0.0), axis=1, keepdims=True)

    def bookkeeping():
        pivots_copy.wait()
        pivot_row = pivots_ref[...].astype(F32)
        pivot_col = column(pivot_row)
        chosen = jnp.max(jnp.where(pivot_col == jj.astype(F32), 1.0, 0.0), axis=0, keepdims=True)
        free = 1.0 - chosen
        far = jnp.where(pivot_row >= block, 1.0, 0.0)
        which = iota((16, block), 0)
        both = jnp.where(which == 0, free, jnp.where(which == 1, far, 0.0))
        ranks = dot(both.astype(BF16), jnp.where(ii < jj, 1.0, 0.0).astype(BF16))
        far_rank = column(ranks[1:2])
        match = (free > 0.5) & (ranks[0:1] == far_rank)
        source = jnp.sum(jnp.where(match, jj.astype(F32), 0.0), axis=1, keepdims=True)
        state.update(pivot_row=pivot_row, pivot_col=pivot_col, source=source)

    def pick():
        pivot_col, source = state["pivot_col"], state["source"]
        first = (me_r * rows).astype(F32)
        mine = (pivot_col >= first) & (pivot_col < first + rows)
        holds = lead.astype(F32)
        index = jnp.where(mine, pivot_col - first, source * holds - (1.0 - holds))
        slab_copy.wait()
        total = jnp.zeros((block, width), F32)
        for start in range(0, rows, block):
            hot = jnp.where((jj + start).astype(F32) == index, 1.0, 0.0).astype(BF16)
            total = total + dot(hot, slab_ref[start:start + block, :])
        picked[...] = total.astype(BF16)

    def core_copy():
        return pltpu.make_async_remote_copy(
            src_ref=picked, dst_ref=picked_in, send_sem=core_sem.at[0], recv_sem=core_sem.at[1],
            device_id=(peer, me_c), device_id_type=MESH,
        )

    def own_homes():
        homes[:, width:] = jnp.ones((block, LANES), BF16)

        @pl.when(me_r == 0)
        def _():
            hot = jnp.where(jj.astype(F32) == state["source"], 1.0, 0.0).astype(BF16)
            homes[:, :width] = dot(hot, slab_ref[:block, :]).astype(BF16)

    half = block // 2

    def chip_copy(step):
        rows_of = pl.ds(pl.multiple_of(core * half, half), half)
        to = ((chip + step) % chips) * 2 + core
        return pltpu.make_async_remote_copy(
            src_ref=merged.at[0, rows_of], dst_ref=merged.at[step, rows_of],
            send_sem=chip_send.at[step - 1], recv_sem=chip_recv.at[step - 1],
            device_id=(to, me_c), device_id_type=MESH,
        )

    def relay_copy(step):
        part = merged.at[step, pl.ds(pl.multiple_of(core * half, half), half)]
        return pltpu.make_async_remote_copy(
            src_ref=part, dst_ref=part, send_sem=relay_send.at[step - 1], recv_sem=relay_recv.at[step - 1],
            device_id=(peer, me_c), device_id_type=MESH,
        )

    def merge():
        core_copy().wait()
        pivot_col = state["pivot_col"]
        holds = (chip == 0).astype(F32)
        second = jnp.where((pivot_col >= rows) & (pivot_col < 2 * rows), holds, 0.0)
        mine, theirs = picked[...].astype(F32), picked_in[...].astype(F32)
        even = (core == 0).astype(F32)
        keep_mine = 1.0 - even * second
        keep_theirs = 1.0 - (1.0 - even) * second
        merged[0] = (mine * keep_mine + theirs * keep_theirs).astype(BF16)
        for step in range(1, chips):
            chip_copy(step).start()

    def relay_chips():
        for step in range(1, chips):
            chip_copy(step).wait()
            relay_copy(step).start()

    def assemble():
        for step in range(1, chips):
            relay_copy(step).wait()
        pivot_col = state["pivot_col"]
        top = jnp.zeros((block, width), F32)
        for step in range(chips):
            low = (((chip + chips - step) % chips) * 2 * rows).astype(F32)
            here = (pivot_col >= low) & (pivot_col < low + 2 * rows)
            top = top + jnp.where(here, merged[step].astype(F32), 0.0)
        state["top"] = top.astype(BF16)

        @pl.when(me_r == 1)
        def _():
            homes[:, :width] = picked_in[...]

        for step in range(1, chips):
            @pl.when((chip > 0) & (chip == step))
            def _():
                homes[:, :width] = merged[step]

    def interchange(start):
        def act():
            row = iota((block, block), 0) + (me_r * rows + start)
            pivot_row = state["pivot_row"]
            hot = jnp.where((row.astype(F32) == pivot_row) & (pivot_row >= block), 1.0, 0.0)
            both = dot(hot.astype(BF16), homes[...])
            taken = both[:, width:] > 0.5
            for lane in range(0, width, LANES):
                kept = slab_ref[start:start + block, lane:lane + LANES].astype(F32)
                new = jnp.where(taken, both[:, lane:lane + LANES], kept)
                pivoted[start:start + block, lane:lane + LANES] = new.astype(BF16)
        return act

    base = min(block, 256)
    small = min(base, 16)
    bi = iota((base, base), 0)
    bj = iota((base, base), 1)
    groups = block // base

    def diagonal(g):
        part = l_top_ref[g * base:(g + 1) * base, g * base:(g + 1) * base].astype(F32)
        return jnp.where(bi > bj, part, 0.0)

    def start_inverse():
        l_top_copy.wait()
        state["x"], state["power"] = [], []
        for g in range(groups):
            near = jnp.where(bi // small == bj // small, diagonal(g), 0.0)
            state["x"].append(jnp.where(bi == bj, 1.0, 0.0) - near)
            exact = near.astype(BF16)
            state["power"].append(dot(exact, exact))

    def power_step():
        for g in range(groups):
            x, power = state["x"][g], state["power"][g]
            state["x"][g] = x + dot_split(x, power)
            state["power"][g] = dot_split(power, power)

    def last_power():
        for g in range(groups):
            x, power = state["x"][g], state["power"][g]
            state["x"][g] = x + dot_split(x, power)

    def double(size):
        def act():
            for g in range(groups):
                link = jnp.where(
                    (bi // (2 * size) == bj // (2 * size)) & (bi // size != bj // size), diagonal(g), 0.0
                )
                inv = state["x"][g]
                state["x"][g] = inv - dot_split(inv, dot_exact_left(link.astype(BF16), inv))
        return act

    def join():
        for g in range(groups):
            high[g * base:(g + 1) * base, :] = jnp.zeros((base, block), F32)
            high[g * base:(g + 1) * base, g * base:(g + 1) * base] = state["x"][g]

    def join_double(size):
        def act():
            for at in range(0, block, 2 * size):
                a = high[at:at + size, at:at + size]
                b = high[at + size:at + 2 * size, at + size:at + 2 * size]
                c = l_top_ref[at + size:at + 2 * size, at:at + size]
                high[at + size:at + 2 * size, at:at + size] = -dot_split(b, dot_exact_left(c, a))
        return act

    def split():
        inverse_hi[...], inverse_lo[...] = halves(high[...])

    def solve():
        top = state["top"]
        u_ref[...] = (dot(inverse_hi[...], top) + dot(inverse_lo[...], top)).astype(BF16)

    inverse = [start_inverse]
    size = 4
    while size < small:
        inverse.append(power_step)
        size *= 2
    if small > 2:
        inverse.append(last_power)
    size = small
    while size < base:
        inverse.append(double(size))
        size *= 2
    inverse.append(join)
    while size < block:
        inverse.append(join_double(size))
        size *= 2
    inverse.append(split)

    def update(piece):
        start, size = pieces[piece]

        def act():
            panel = gathered[:, :, start:start + size].reshape(block, size).astype(BF16)
            out_ref[start:start + size, :] = trailing(panel, u_ref[...], pivoted[start:start + size, :])

        needed(piece, act)
        if start < block:
            @pl.when(lead)
            def _():
                end = min(block, start + size)
                out_ref[start:end, :] = u_ref[start:end, :]

    pl.semaphore_wait(barrier, 1 + chips + has_below + has_above)
    panel_copy.wait()
    first_sends()
    tell(0)
    bookkeeping()
    pick()
    core_copy().start()
    told(0)
    tell(1)

    own_homes()

    def relays(distance):
        return [relay(distance, piece) for piece in bulk] if distance < length else []

    changes = [interchange(start) for start in range(0, rows, block)]
    plan = inverse[:3] + [merge, guest_own] + weave(relays(1), inverse[3:6])
    plan += [other_rest, own_rest(0, other), own_rest(1, x), own_rest(1, other)] + inverse[6:8]
    second = relays(2)
    half_way = len(second) // 2
    plan += weave(second[:half_way], inverse[8:10]) + [guest_line, pass_rest(1, 1)]
    plan += weave(second[half_way:], [relay_chips] + inverse[10:])
    plan += [own_rest(2, x), own_rest(2, other), pass_rest(2, 1), assemble, solve]
    plan += weave(relays(3), changes[:3] + [pass_rest(2, 2)]) + changes[3:] + [guest_other]
    for distance in range(3, length):
        plan += relays(distance) if distance > 3 else []
        plan += [own_rest(distance, x), own_rest(distance, other)]
        plan += [pass_rest(distance, reach) for reach in range(1, distance + 1)]
    for act in plan:
        act()

    for piece in bulk:
        if piece == 0:
            for distance in range(1, length - 1):
                last_rests(distance)
            start, size = columns_of(rest, False)
            total = pivoted[start:start + size, :].astype(F32)
            last = last_level(length)
            for step in range(1, length):
                total = total - level_of(gathered, u_ref, (last + step) % length, (start, size))
            partial[...] = total
        crossed(piece)
        if piece < tail:
            update(piece)
    last_rests(length - 1)
    guest_last()

    drain()


def finish(done_ref, gathered, u_ref, partial, pivoted, out_hbm, result, sem):
    block = u_ref.shape[0]
    edge = cuts(gathered.shape[2])[-2][0]
    start, size = cuts(gathered.shape[2], False)[-1]

    def store(source, start, size, n):
        copy = pltpu.make_async_copy(source, out_hbm.at[pl.ds(start, size)], sem.at[n])
        copy.start()
        return copy

    copies = [store(done_ref.at[pl.ds(0, edge)], 0, edge, 0)]
    panel = gathered[:, :, edge:start].reshape(block, start - edge).astype(BF16)
    result[:start - edge, :] = trailing(panel, u_ref[...], pivoted[edge:start, :])
    copies.append(store(result.at[pl.ds(0, start - edge)], edge, start - edge, 2))
    last = last_level(gathered.shape[0] // 2)
    result[start - edge:, :] = (partial[...] - level_of(gathered, u_ref, last, (start, size))).astype(BF16)
    copies.append(store(result.at[pl.ds(start - edge, size)], start, size, 1))
    for copy in copies:
        copy.wait()


def per_device(n_prow, n_pcol, slab, pivots, l_top, l_panel_t):
    rows, width = slab.shape
    block = pivots.shape[0]
    depth = l_panel_t.shape[0]
    kind = BF16 if depth % 16 == 0 else F32
    panel = l_panel_t.astype(kind)
    chips = n_prow // 2
    n_pieces = len(cuts(rows))
    vmem = pl.BlockSpec(memory_space=pltpu.VMEM)
    anywhere = pl.BlockSpec(memory_space=pltpu.HBM)
    dma = pltpu.SemaphoreType.DMA
    kept = [
        pltpu.VMEM((rows, width), BF16),
        pltpu.VMEM((n_pcol, depth, rows), kind),
        pltpu.VMEM((block, width), BF16),
        pltpu.VMEM((cuts(rows, False)[-1][1], width), F32),
        pltpu.VMEM((rows, width), BF16),
    ]
    done, gathered, u, partial, pivoted = pl.pallas_call(
        functools.partial(kernel, n_prow, n_pcol),
        out_shape=kept,
        in_specs=[anywhere] * 4,
        out_specs=[vmem] * 5,
        scratch_shapes=[
            pltpu.VMEM((rows, width), BF16),
            pltpu.VMEM((1, block), jnp.int32),
            pltpu.VMEM((block, block), BF16),
            pltpu.VMEM((block, width), BF16),
            pltpu.VMEM((block, width), BF16),
            pltpu.VMEM((chips, block, width), BF16),
            pltpu.VMEM((block, width + LANES), BF16),
            pltpu.VMEM((block, block), BF16),
            pltpu.VMEM((block, block), BF16),
            pltpu.VMEM((block, block), F32),
            pltpu.VMEM((n_pcol, depth, LANES), kind),
            dma((4,)),
            dma((n_pcol // 2, n_pieces - 1)),
            dma((n_pieces - 1,)),
            dma((n_pcol // 2,)),
            dma((6,)),
            dma((5,)),
            pltpu.SemaphoreType.REGULAR((2,)),
            dma((2,)),
            dma((chips - 1,)),
            dma((chips - 1,)),
            dma((chips - 1,)),
            dma((chips - 1,)),
        ],
        compiler_params=pltpu.CompilerParams(collective_id=0, has_side_effects=True, vmem_limit_bytes=LIMIT),
    )(slab, pivots.reshape(1, block), l_top, panel)
    return pl.pallas_call(
        finish,
        out_shape=pltpu.HBM((rows, width), BF16),
        in_specs=[vmem] * 5,
        out_specs=anywhere,
        scratch_shapes=[pltpu.VMEM((rows - cuts(rows)[-2][0], width), BF16), dma((3,))],
        compiler_params=pltpu.CompilerParams(vmem_limit_bytes=16 * 2**20),
    )(done, gathered, u, partial, pivoted)


def solution(mesh):
    return jax.shard_map(
        functools.partial(per_device, mesh.shape["prow"], mesh.shape["pcol"]),
        mesh=mesh,
        in_specs=(P("prow", "pcol"), P(), P(), P("pcol", "prow")),
        out_specs=P("prow", "pcol"),
        check_vma=False,
    )
```

```python
import functools

import jax
import jax.numpy as jnp
from jax import lax
from jax.experimental import pallas as pl
from jax.experimental.pallas import tpu as pltpu
from jax.sharding import PartitionSpec as P

MESH = pl.DeviceIdType.MESH
F32 = jnp.float32
BF16 = jnp.bfloat16
LANES = 128


def dot(a, b):
    return jnp.dot(a, b, preferred_element_type=F32)


def iota(shape, axis):
    return lax.broadcasted_iota(jnp.int32, shape, axis)


def halves(a):
    high = a.astype(BF16)
    return high, (a - high.astype(F32)).astype(BF16)


def dot_exact_left(a, b):
    high, low = halves(b)
    return dot(a, high) + dot(a, low)


def dot_split(a, b):
    a_high, a_low = halves(a)
    b_high, b_low = halves(b)
    return dot(a_high, b_high) + (dot(a_high, b_low) + dot(a_low, b_high))


STRIPS = (0, 4, 7, 10)
THICK = 12
THIN = 14
LIMIT = 54 * 2**20


def cuts(width, thick=True):
    units = width // LANES
    edges = [units * part // 16 * LANES for part in STRIPS + (THICK if thick else THIN, 16)]
    return [(a, b - a) for a, b in zip(edges[:-1], edges[1:])]


def box(columns, shape):
    for count in range(1, shape[0] + 1):
        if columns % (count * LANES) == 0 and columns // count <= shape[2]:
            return count, columns // count


def level_of(gathered, u_ref, level, columns):
    depth = 2 * gathered.shape[1]
    panel = gathered[pl.ds(level * 2, 2), :, columns[0]:columns[0] + columns[1]].reshape(depth, columns[1])
    return lax.dot_general(
        panel.astype(BF16), u_ref[pl.ds(pl.multiple_of(level * depth, depth), depth), :],
        (((0,), (0,)), ((), ())), preferred_element_type=F32,
    )


def last_level(length):
    z = lax.axis_index("pcol") // 2
    return jnp.where(z < length // 2, length - 1, 0)


def weave(events, work):
    plan, count = [], max(1, len(events))
    for at, event in enumerate(events):
        plan += [event] + work[at * len(work) // count:(at + 1) * len(work) // count]
    return plan


def trailing(panel, u, rows):
    product = lax.dot_general(panel, u, (((0,), (0,)), ((), ())), preferred_element_type=F32)
    return (rows.astype(F32) - product).astype(BF16)


def kernel(
    n_prow, n_pcol,
    slab_hbm, pivots_hbm, l_top_hbm, panel_hbm, out_ref, gathered, u_ref, partial, pivoted,
    slab_ref, pivots_ref, l_top_ref, picked, picked_in, merged, homes, inverse_hi, inverse_lo, high, guest,
    local_sem, line_recv, cross_recv, rest_recv, sent, guest_sem, ready, core_sem, chip_send, chip_recv, relay_send, relay_recv,
):
    block = l_top_ref.shape[0]
    rows, width = slab_ref.shape
    me_r = lax.axis_index("prow")
    me_c = lax.axis_index("pcol")
    chips = n_prow // 2
    chip, core = me_r // 2, me_r % 2
    peer = me_r + 1 - 2 * core
    length = n_pcol // 2
    z, x = me_c // 2, me_c % 2
    other = 1 - x
    pieces = cuts(gathered.shape[2])
    bulk = range(len(pieces) - 1)
    rest = len(pieces) - 1
    lead = me_r == 0

    def needed(piece, act):
        start, size = pieces[piece]
        if start + size <= block:
            pl.when(jnp.logical_not(lead))(act)
        else:
            act()

    panel_copy = pltpu.make_async_copy(panel_hbm, gathered.at[me_c], local_sem.at[0])
    pivots_copy = pltpu.make_async_copy(pivots_hbm, pivots_ref, local_sem.at[1])
    slab_copy = pltpu.make_async_copy(slab_hbm, slab_ref, local_sem.at[2])
    l_top_copy = pltpu.make_async_copy(l_top_hbm, l_top_ref, local_sem.at[3])

    barrier = pltpu.get_barrier_semaphore()

    def greet(r, c):
        pl.semaphore_signal(barrier, inc=1, device_id=(r, c), device_id_type=MESH)

    greet(me_r, z * 2 + other)

    @pl.when(z > 0)
    def _():
        greet(me_r, me_c - 2)

    @pl.when(z < length - 1)
    def _():
        greet(me_r, me_c + 2)

    for step in range(1, chips):
        greet(((chip + step) % chips) * 2 + core, me_c)
    greet(peer, me_c)

    panel_copy.start()
    pivots_copy.start()
    slab_copy.start()
    l_top_copy.start()

    has_below = (z + length - 1) // length
    has_above = (2 * length - 2 - z) // length

    tail = rest - 1
    mixed = length == 4
    moves = n_prow == 4 and length <= 4
    giver = me_r == 2

    def by_class(at, act):
        if mixed:
            outer = ((at == 0) | (at == length - 1)) & jnp.logical_not(lead)
            pl.when(outer)(lambda: act(True))
            pl.when(jnp.logical_not(outer))(lambda: act(False))
        else:
            act(True)

    def columns_of(piece, kind):
        thick, given = kind if isinstance(kind, tuple) else (kind, False)
        start, size = cuts(gathered.shape[2], thick)[piece]
        return (start + LANES, size - LANES) if given and piece == tail else (start, size)

    def send(source, columns, send_sem, recv_sem, target):
        part = gathered.at[source, :, pl.ds(*columns)]
        pltpu.make_async_remote_copy(
            src_ref=part, dst_ref=part, send_sem=send_sem, recv_sem=recv_sem,
            device_id=(me_r, target), device_id_type=MESH,
        ).start()

    def arrival(columns, send_sem, recv_sem):
        count, size = box(columns, gathered.shape)
        part = gathered.at[pl.ds(0, count), :, pl.ds(0, size)]
        return pltpu.make_async_remote_copy(
            src_ref=part, dst_ref=part, send_sem=send_sem, recv_sem=recv_sem,
            device_id=(me_r, z * 2 + other), device_id_type=MESH,
        )

    def landed(columns, recv_sem):
        arrival(columns, sent.at[0], recv_sem).wait_recv()

    def neighbour(way):
        return me_c + 2 - 4 * way

    def slot(at, level):
        return at - (at > level).astype(jnp.int32)

    def line(way, at, piece, thick):
        send(
            at * 2 + x, columns_of(piece, thick), sent.at[way if piece < 2 else 2 + way], line_recv.at[slot(at, z + 1 - 2 * way), piece],
            neighbour(way),
        )

    def cross(at, piece, thick):
        send(at * 2 + x, columns_of(piece, thick), sent.at[4], cross_recv.at[piece], z * 2 + other)

    def line_rest(way, at, side, thick):
        send(at * 2 + side, columns_of(rest, thick), sent.at[2 + way], rest_recv.at[at], neighbour(way))

    def classed(at, piece, act):
        if piece == tail and moves:
            pl.when(giver)(lambda: by_class(at, lambda thick: act((thick, True))))
            pl.when(jnp.logical_not(giver))(lambda: by_class(at, act))
        elif piece >= tail:
            by_class(at, act)
        else:
            act(True)

    def both_ways(act):
        pl.when(z < length - 1)(lambda: act(0))
        pl.when(z > 0)(lambda: act(1))

    moved = pl.ds(pieces[tail][0], LANES)

    def guest_copy(source, target, recv_sem, row, column):
        return pltpu.make_async_remote_copy(
            src_ref=source, dst_ref=target, send_sem=guest_sem.at[4], recv_sem=recv_sem,
            device_id=(row, column), device_id_type=MESH,
        )

    def guest_total(count, recv_sem):
        rows_of, size = box(count * LANES, gathered.shape)
        part = gathered.at[pl.ds(0, rows_of), :, pl.ds(0, size)]
        return guest_copy(part, part, recv_sem, me_r, z * 2 + other)

    def only(who):
        return lambda act: pl.when(who)(act) if moves else None

    def guest_give():
        @only(giver)
        def _():
            guest_copy(gathered.at[me_c, :, moved], guest.at[me_c], guest_sem.at[0], 0, me_c).start()

    def guest_cross(source):
        part = guest.at[source]
        guest_copy(part, part, guest_sem.at[2], me_r, z * 2 + other).start()

    def guest_home(source):
        guest_copy(guest.at[source], gathered.at[source, :, moved], guest_sem.at[3], 2, me_c).start()

    def tell(n):
        @only(lead)
        def _():
            both_ways(lambda way: pl.semaphore_signal(
                ready.at[n], inc=1, device_id=(0, neighbour(way)), device_id_type=MESH
            ))

    def told(n):
        @only(lead)
        def _():
            pl.semaphore_wait(ready.at[n], has_below + has_above)

    def guest_own():
        told(1)

        @only(lead)
        def _():
            guest_total(1, guest_sem.at[0]).wait_recv()
            part = guest.at[me_c]
            for step in range(1, length):
                guest_copy(part, part, guest_sem.at[1], me_r, (z + step) % length * 2 + x).start()
            guest_cross(me_c)

    def guest_line():
        @only(lead)
        def _():
            guest_total(length - 1, guest_sem.at[1]).wait_recv()
            for step in range(1, length):
                guest_cross((z + step) % length * 2 + x)
            for step in range(1, length):
                guest_home((z + step) % length * 2 + x)

    def guest_other():
        @only(lead)
        def _():
            guest_total(length, guest_sem.at[2]).wait_recv()
            for at in range(length):
                guest_home(at * 2 + other)

    def guest_last():
        @only(giver)
        def _():
            guest_total(2 * length - 1, guest_sem.at[3]).wait_recv()

    def guest_drain():
        @only(giver)
        def _():
            guest_total(1, guest_sem.at[3]).wait_send()

        @only(lead)
        def _():
            guest_total(4 * length - 2, guest_sem.at[3]).wait_send()

    def first_sends():
        guest_give()
        for piece in bulk:
            def own(thick):
                both_ways(lambda way: line(way, z, piece, thick))
                cross(z, piece, thick)
            needed(piece, lambda: classed(z, piece, own))
            if piece == 2:
                by_class(z, lambda thick: send(
                    me_c, columns_of(rest, thick), sent.at[5], rest_recv.at[z], z * 2 + other
                ))
        own_rest(0, x)()

    def rest_ways(distance, act):
        if distance < length - 1:
            pl.when(z == distance)(lambda: act(0))
            pl.when(z == length - 1 - distance)(lambda: act(1))

    def own_rest(distance, side):
        def act(way):
            by_class(z, lambda thick: line_rest(way, z, side, thick))
        return lambda: rest_ways(distance, act)

    def other_rest():
        by_class(z, lambda thick: landed(columns_of(rest, thick)[1], rest_recv.at[z]))

    def both_rests(at, act=None):
        def classed_act(thick):
            landed(2 * columns_of(rest, thick)[1], rest_recv.at[at])
            if act is not None:
                for side in (0, 1):
                    act(side, thick)
        by_class(at, classed_act)

    def pass_rest(distance, reach):
        def onward(way):
            at = z + (2 * way - 1) * reach
            both_rests(at, lambda side, thick: line_rest(way, at, side, thick))
        return lambda: rest_ways(distance, onward)

    def relay(distance, piece):
        def both():
            for way, at, reached, onward in (
                (0, z - distance, z >= distance, z < length - 1),
                (1, z + distance, z < length - distance, z > 0),
            ):
                def pass_on(thick):
                    landed(columns_of(piece, thick)[1], line_recv.at[slot(at, z), piece])
                    pl.when(onward)(lambda: line(way, at, piece, thick))
                    cross(at, piece, thick)

                pl.when(reached)(lambda: classed(at, piece, pass_on))
        return lambda: needed(piece, both)

    def last_rests(distance):
        for way, at, reached in (
            (0, z - distance, (z >= distance) & (z == length - 1)),
            (1, z + distance, (z < length - distance) & (z == 0)),
        ):
            pl.when(reached)(lambda: both_rests(at))

    def lanes_of(pieces_of, levels, kind):
        leading, given = kind
        total = 0
        for at in levels:
            thick = not mixed or (not leading and at in (0, length - 1))
            for piece in pieces_of:
                start, size = columns_of(piece, (thick, given))
                total += 0 if leading and start + size <= block else size
        return total

    def for_kinds(act):
        pl.when(lead)(lambda: act((True, False)))
        if moves:
            pl.when(giver)(lambda: act((False, True)))
            pl.when(jnp.logical_not(lead | giver))(lambda: act((False, False)))
        else:
            pl.when(jnp.logical_not(lead))(lambda: act((False, False)))

    def crossed(piece):
        if piece == tail:
            for_kinds(lambda kind: landed(lanes_of([tail], range(length), kind), cross_recv.at[tail]))
        else:
            needed(piece, lambda: landed(length * pieces[piece][1], cross_recv.at[piece]))

    def drain():
        def gone(sem, columns):
            arrival(columns, sent.at[sem], rest_recv.at[0]).wait_send()

        def act(kind):
            for at in range(length):
                def here():
                    if at < length - 1:
                        gone(0, lanes_of(range(2), range(at + 1), kind))
                        gone(2, lanes_of([*range(2, rest), rest, rest], range(at + 1), kind))
                    if at > 0:
                        gone(1, lanes_of(range(2), range(at, length), kind))
                        gone(3, lanes_of([*range(2, rest), rest, rest], range(at, length), kind))
                    gone(5, lanes_of([rest], [at], kind))
                pl.when(z == at)(here)
            gone(4, lanes_of(bulk, range(length), kind))

        for_kinds(act)
        guest_drain()

    state = {}
    ii = iota((block, block), 0)
    jj = iota((block, block), 1)

    def column(row):
        return jnp.sum(jnp.where(ii == jj, row, 0.0), axis=1, keepdims=True)

    def bookkeeping():
        pivots_copy.wait()
        pivot_row = pivots_ref[...].astype(F32)
        pivot_col = column(pivot_row)
        chosen = jnp.max(jnp.where(pivot_col == jj.astype(F32), 1.0, 0.0), axis=0, keepdims=True)
        free = 1.0 - chosen
        far = jnp.where(pivot_row >= block, 1.0, 0.0)
        which = iota((16, block), 0)
        both = jnp.where(which == 0, free, jnp.where(which == 1, far, 0.0))
        ranks = dot(both.astype(BF16), jnp.where(ii < jj, 1.0, 0.0).astype(BF16))
        far_rank = column(ranks[1:2])
        match = (free > 0.5) & (ranks[0:1] == far_rank)
        source = jnp.sum(jnp.where(match, jj.astype(F32), 0.0), axis=1, keepdims=True)
        state.update(pivot_row=pivot_row, pivot_col=pivot_col, source=source)

    def pick():
        pivot_col, source = state["pivot_col"], state["source"]
        first = (me_r * rows).astype(F32)
        mine = (pivot_col >= first) & (pivot_col < first + rows)
        holds = lead.astype(F32)
        index = jnp.where(mine, pivot_col - first, source * holds - (1.0 - holds))
        slab_copy.wait()
        total = jnp.zeros((block, width), F32)
        for start in range(0, rows, block):
            hot = jnp.where((jj + start).astype(F32) == index, 1.0, 0.0).astype(BF16)
            total = total + dot(hot, slab_ref[start:start + block, :])
        picked[...] = total.astype(BF16)

    def core_copy():
        return pltpu.make_async_remote_copy(
            src_ref=picked, dst_ref=picked_in, send_sem=core_sem.at[0], recv_sem=core_sem.at[1],
            device_id=(peer, me_c), device_id_type=MESH,
        )

    def own_homes():
        homes[:, width:] = jnp.ones((block, LANES), BF16)

        @pl.when(me_r == 0)
        def _():
            hot = jnp.where(jj.astype(F32) == state["source"], 1.0, 0.0).astype(BF16)
            homes[:, :width] = dot(hot, slab_ref[:block, :]).astype(BF16)

    half = block // 2

    def chip_copy(step):
        rows_of = pl.ds(pl.multiple_of(core * half, half), half)
        to = ((chip + step) % chips) * 2 + core
        return pltpu.make_async_remote_copy(
            src_ref=merged.at[0, rows_of], dst_ref=merged.at[step, rows_of],
            send_sem=chip_send.at[step - 1], recv_sem=chip_recv.at[step - 1],
            device_id=(to, me_c), device_id_type=MESH,
        )

    def relay_copy(step):
        part = merged.at[step, pl.ds(pl.multiple_of(core * half, half), half)]
        return pltpu.make_async_remote_copy(
            src_ref=part, dst_ref=part, send_sem=relay_send.at[step - 1], recv_sem=relay_recv.at[step - 1],
            device_id=(peer, me_c), device_id_type=MESH,
        )

    def merge():
        core_copy().wait()
        pivot_col = state["pivot_col"]
        holds = (chip == 0).astype(F32)
        second = jnp.where((pivot_col >= rows) & (pivot_col < 2 * rows), holds, 0.0)
        mine, theirs = picked[...].astype(F32), picked_in[...].astype(F32)
        even = (core == 0).astype(F32)
        keep_mine = 1.0 - even * second
        keep_theirs = 1.0 - (1.0 - even) * second
        merged[0] = (mine * keep_mine + theirs * keep_theirs).astype(BF16)
        for step in range(1, chips):
            chip_copy(step).start()

    def relay_chips():
        for step in range(1, chips):
            chip_copy(step).wait()
            relay_copy(step).start()

    def assemble():
        for step in range(1, chips):
            relay_copy(step).wait()
        pivot_col = state["pivot_col"]
        top = jnp.zeros((block, width), F32)
        for step in range(chips):
            low = (((chip + chips - step) % chips) * 2 * rows).astype(F32)
            here = (pivot_col >= low) & (pivot_col < low + 2 * rows)
            top = top + jnp.where(here, merged[step].astype(F32), 0.0)
        state["top"] = top.astype(BF16)

        @pl.when(me_r == 1)
        def _():
            homes[:, :width] = picked_in[...]

        for step in range(1, chips):
            @pl.when((chip > 0) & (chip == step))
            def _():
                homes[:, :width] = merged[step]

    def interchange(start):
        def act():
            row = iota((block, block), 0) + (me_r * rows + start)
            pivot_row = state["pivot_row"]
            hot = jnp.where((row.astype(F32) == pivot_row) & (pivot_row >= block), 1.0, 0.0)
            both = dot(hot.astype(BF16), homes[...])
            taken = both[:, width:] > 0.5
            for lane in range(0, width, LANES):
                kept = slab_ref[start:start + block, lane:lane + LANES].astype(F32)
                new = jnp.where(taken, both[:, lane:lane + LANES], kept)
                pivoted[start:start + block, lane:lane + LANES] = new.astype(BF16)
        return act

    base = min(block, 256)
    small = min(base, 16)
    bi = iota((base, base), 0)
    bj = iota((base, base), 1)
    groups = block // base

    def diagonal(g):
        part = l_top_ref[g * base:(g + 1) * base, g * base:(g + 1) * base].astype(F32)
        return jnp.where(bi > bj, part, 0.0)

    def start_inverse():
        l_top_copy.wait()
        state["x"], state["power"] = [], []
        for g in range(groups):
            near = jnp.where(bi // small == bj // small, diagonal(g), 0.0)
            state["x"].append(jnp.where(bi == bj, 1.0, 0.0) - near)
            exact = near.astype(BF16)
            state["power"].append(dot(exact, exact))

    def power_step():
        for g in range(groups):
            x, power = state["x"][g], state["power"][g]
            state["x"][g] = x + dot_split(x, power)
            state["power"][g] = dot_split(power, power)

    def last_power():
        for g in range(groups):
            x, power = state["x"][g], state["power"][g]
            state["x"][g] = x + dot_split(x, power)

    def double(size):
        def act():
            for g in range(groups):
                link = jnp.where(
                    (bi // (2 * size) == bj // (2 * size)) & (bi // size != bj // size), diagonal(g), 0.0
                )
                inv = state["x"][g]
                state["x"][g] = inv - dot_split(inv, dot_exact_left(link.astype(BF16), inv))
        return act

    def join():
        for g in range(groups):
            high[g * base:(g + 1) * base, :] = jnp.zeros((base, block), F32)
            high[g * base:(g + 1) * base, g * base:(g + 1) * base] = state["x"][g]

    def join_double(size):
        def act():
            for at in range(0, block, 2 * size):
                a = high[at:at + size, at:at + size]
                b = high[at + size:at + 2 * size, at + size:at + 2 * size]
                c = l_top_ref[at + size:at + 2 * size, at:at + size]
                high[at + size:at + 2 * size, at:at + size] = -dot_split(b, dot_exact_left(c, a))
        return act

    def split():
        inverse_hi[...], inverse_lo[...] = halves(high[...])

    def solve():
        top = state["top"]
        u_ref[...] = (dot(inverse_hi[...], top) + dot(inverse_lo[...], top)).astype(BF16)

    inverse = [start_inverse]
    size = 4
    while size < small:
        inverse.append(power_step)
        size *= 2
    if small > 2:
        inverse.append(last_power)
    size = small
    while size < base:
        inverse.append(double(size))
        size *= 2
    inverse.append(join)
    while size < block:
        inverse.append(join_double(size))
        size *= 2
    inverse.append(split)

    def update(piece):
        start, size = pieces[piece]

        def act():
            panel = gathered[:, :, start:start + size].reshape(block, size).astype(BF16)
            out_ref[start:start + size, :] = trailing(panel, u_ref[...], pivoted[start:start + size, :])

        needed(piece, act)
        if start < block:
            @pl.when(lead)
            def _():
                end = min(block, start + size)
                out_ref[start:end, :] = u_ref[start:end, :]

    pl.semaphore_wait(barrier, 1 + chips + has_below + has_above)
    panel_copy.wait()
    first_sends()
    tell(0)
    bookkeeping()
    pick()
    core_copy().start()
    told(0)
    tell(1)

    own_homes()

    def relays(distance):
        return [relay(distance, piece) for piece in bulk] if distance < length else []

    changes = [interchange(start) for start in range(0, rows, block)]
    plan = inverse[:3] + [merge, guest_own] + weave(relays(1), inverse[3:6])
    plan += [other_rest, own_rest(0, other), own_rest(1, x), own_rest(1, other)] + inverse[6:8]
    second = relays(2)
    half_way = len(second) // 2
    plan += weave(second[:half_way], inverse[8:10]) + [guest_line, pass_rest(1, 1)]
    plan += weave(second[half_way:], [relay_chips] + inverse[10:])
    plan += [own_rest(2, x), own_rest(2, other), pass_rest(2, 1), assemble, solve]
    plan += weave(relays(3), changes[:3] + [pass_rest(2, 2)]) + changes[3:] + [guest_other]
    for distance in range(3, length):
        plan += relays(distance) if distance > 3 else []
        plan += [own_rest(distance, x), own_rest(distance, other)]
        plan += [pass_rest(distance, reach) for reach in range(1, distance + 1)]
    for act in plan:
        act()

    def near_levels():
        for distance in range(1, length - 1):
            last_rests(distance)
        start, size = columns_of(rest, False)
        total = pivoted[start:start + size, :].astype(F32)
        last = last_level(length)
        for step in range(1, length):
            total = total - level_of(gathered, u_ref, (last + step) % length, (start, size))
        partial[...] = total

    for piece in bulk:
        if piece == 0:
            pl.when(jnp.logical_not(lead))(near_levels)
        if piece == tail - 1:
            pl.when(lead)(near_levels)
        crossed(piece)
        if piece < tail:
            update(piece)
    last_rests(length - 1)
    guest_last()

    drain()


def finish(done_ref, gathered, u_ref, partial, pivoted, out_hbm, result, sem):
    block = u_ref.shape[0]
    edge = cuts(gathered.shape[2])[-2][0]
    start, size = cuts(gathered.shape[2], False)[-1]

    def store(source, start, size, n):
        copy = pltpu.make_async_copy(source, out_hbm.at[pl.ds(start, size)], sem.at[n])
        copy.start()
        return copy

    copies = [store(done_ref.at[pl.ds(0, edge)], 0, edge, 0)]
    panel = gathered[:, :, edge:start].reshape(block, start - edge).astype(BF16)
    result[:start - edge, :] = trailing(panel, u_ref[...], pivoted[edge:start, :])
    copies.append(store(result.at[pl.ds(0, start - edge)], edge, start - edge, 2))
    last = last_level(gathered.shape[0] // 2)
    result[start - edge:, :] = (partial[...] - level_of(gathered, u_ref, last, (start, size))).astype(BF16)
    copies.append(store(result.at[pl.ds(start - edge, size)], start, size, 1))
    for copy in copies:
        copy.wait()


def per_device(n_prow, n_pcol, slab, pivots, l_top, l_panel_t):
    rows, width = slab.shape
    block = pivots.shape[0]
    depth = l_panel_t.shape[0]
    kind = BF16 if depth % 16 == 0 else F32
    panel = l_panel_t.astype(kind)
    chips = n_prow // 2
    n_pieces = len(cuts(rows))
    vmem = pl.BlockSpec(memory_space=pltpu.VMEM)
    anywhere = pl.BlockSpec(memory_space=pltpu.HBM)
    dma = pltpu.SemaphoreType.DMA
    kept = [
        pltpu.VMEM((rows, width), BF16),
        pltpu.VMEM((n_pcol, depth, rows), kind),
        pltpu.VMEM((block, width), BF16),
        pltpu.VMEM((cuts(rows, False)[-1][1], width), F32),
        pltpu.VMEM((rows, width), BF16),
    ]
    done, gathered, u, partial, pivoted = pl.pallas_call(
        functools.partial(kernel, n_prow, n_pcol),
        out_shape=kept,
        in_specs=[anywhere] * 4,
        out_specs=[vmem] * 5,
        scratch_shapes=[
            pltpu.VMEM((rows, width), BF16),
            pltpu.VMEM((1, block), jnp.int32),
            pltpu.VMEM((block, block), BF16),
            pltpu.VMEM((block, width), BF16),
            pltpu.VMEM((block, width), BF16),
            pltpu.VMEM((chips, block, width), BF16),
            pltpu.VMEM((block, width + LANES), BF16),
            pltpu.VMEM((block, block), BF16),
            pltpu.VMEM((block, block), BF16),
            pltpu.VMEM((block, block), F32),
            pltpu.VMEM((n_pcol, depth, LANES), kind),
            dma((4,)),
            dma((n_pcol // 2 - 1, n_pieces - 1)),
            dma((n_pieces - 1,)),
            dma((n_pcol // 2,)),
            dma((6,)),
            dma((5,)),
            pltpu.SemaphoreType.REGULAR((2,)),
            dma((2,)),
            dma((chips - 1,)),
            dma((chips - 1,)),
            dma((chips - 1,)),
            dma((chips - 1,)),
        ],
        compiler_params=pltpu.CompilerParams(collective_id=0, has_side_effects=True, vmem_limit_bytes=LIMIT),
    )(slab, pivots.reshape(1, block), l_top, panel)
    return pl.pallas_call(
        finish,
        out_shape=pltpu.HBM((rows, width), BF16),
        in_specs=[vmem] * 5,
        out_specs=anywhere,
        scratch_shapes=[pltpu.VMEM((rows - cuts(rows)[-2][0], width), BF16), dma((3,))],
        compiler_params=pltpu.CompilerParams(vmem_limit_bytes=16 * 2**20),
    )(done, gathered, u, partial, pivoted)


def solution(mesh):
    return jax.shard_map(
        functools.partial(per_device, mesh.shape["prow"], mesh.shape["pcol"]),
        mesh=mesh,
        in_specs=(P("prow", "pcol"), P(), P(), P("pcol", "prow")),
        out_specs=P("prow", "pcol"),
        check_vma=False,
    )
```

```python
import functools

import jax
import jax.numpy as jnp
from jax import lax
from jax.experimental import pallas as pl
from jax.experimental.pallas import tpu as pltpu
from jax.sharding import PartitionSpec as P

MESH = pl.DeviceIdType.MESH
F32 = jnp.float32
BF16 = jnp.bfloat16
LANES = 128


def dot(a, b):
    return jnp.dot(a, b, preferred_element_type=F32)


def iota(shape, axis):
    return lax.broadcasted_iota(jnp.int32, shape, axis)


def halves(a):
    high = a.astype(BF16)
    return high, (a - high.astype(F32)).astype(BF16)


def dot_exact_left(a, b):
    high, low = halves(b)
    return dot(a, high) + dot(a, low)


def dot_split(a, b):
    a_high, a_low = halves(a)
    b_high, b_low = halves(b)
    return dot(a_high, b_high) + (dot(a_high, b_low) + dot(a_low, b_high))


STRIPS = (0, 4, 7, 10)
THICK = 12
THIN = 14
LIMIT = 54 * 2**20


def cuts(width, thick=True):
    units = width // LANES
    edges = [units * part // 16 * LANES for part in STRIPS + (THICK if thick else THIN, 16)]
    return [(a, b - a) for a, b in zip(edges[:-1], edges[1:])]


def box(columns, shape):
    for count in range(1, shape[0] + 1):
        if columns % (count * LANES) == 0 and columns // count <= shape[2]:
            return count, columns // count


def level_of(gathered, u_ref, level, columns):
    depth = 2 * gathered.shape[1]
    panel = gathered[pl.ds(level * 2, 2), :, columns[0]:columns[0] + columns[1]].reshape(depth, columns[1])
    return lax.dot_general(
        panel.astype(BF16), u_ref[pl.ds(pl.multiple_of(level * depth, depth), depth), :],
        (((0,), (0,)), ((), ())), preferred_element_type=F32,
    )


def last_level(length):
    z = lax.axis_index("pcol") // 2
    return jnp.where(z < length // 2, length - 1, 0)


def weave(events, work):
    plan, count = [], max(1, len(events))
    for at, event in enumerate(events):
        plan += [event] + work[at * len(work) // count:(at + 1) * len(work) // count]
    return plan


def trailing(panel, u, rows):
    product = lax.dot_general(panel, u, (((0,), (0,)), ((), ())), preferred_element_type=F32)
    return (rows.astype(F32) - product).astype(BF16)


def kernel(
    n_prow, n_pcol,
    slab_hbm, pivots_hbm, l_top_hbm, panel_hbm, out_ref, gathered, u_ref, partial, pivoted,
    slab_ref, pivots_ref, l_top_ref, picked, picked_in, merged, homes, inverse_hi, inverse_lo, high, guest,
    local_sem, line_recv, cross_recv, rest_recv, sent, guest_sem, ready, core_sem, chip_send, chip_recv, relay_send, relay_recv,
):
    block = l_top_ref.shape[0]
    rows, width = slab_ref.shape
    me_r = lax.axis_index("prow")
    me_c = lax.axis_index("pcol")
    chips = n_prow // 2
    chip, core = me_r // 2, me_r % 2
    peer = me_r + 1 - 2 * core
    length = n_pcol // 2
    z, x = me_c // 2, me_c % 2
    other = 1 - x
    pieces = cuts(gathered.shape[2])
    bulk = range(len(pieces) - 1)
    rest = len(pieces) - 1
    lead = me_r == 0

    def needed(piece, act):
        start, size = pieces[piece]
        if start + size <= block:
            pl.when(jnp.logical_not(lead))(act)
        else:
            act()

    panel_copy = pltpu.make_async_copy(panel_hbm, gathered.at[me_c], local_sem.at[0])
    pivots_copy = pltpu.make_async_copy(pivots_hbm, pivots_ref, local_sem.at[1])
    slab_copy = pltpu.make_async_copy(slab_hbm, slab_ref, local_sem.at[2])
    l_top_copy = pltpu.make_async_copy(l_top_hbm, l_top_ref, local_sem.at[3])

    barrier = pltpu.get_barrier_semaphore()

    def greet(r, c):
        pl.semaphore_signal(barrier, inc=1, device_id=(r, c), device_id_type=MESH)

    greet(me_r, z * 2 + other)

    @pl.when(z > 0)
    def _():
        greet(me_r, me_c - 2)

    @pl.when(z < length - 1)
    def _():
        greet(me_r, me_c + 2)

    for step in range(1, chips):
        greet(((chip + step) % chips) * 2 + core, me_c)
    greet(peer, me_c)

    panel_copy.start()
    pivots_copy.start()
    slab_copy.start()
    l_top_copy.start()

    has_below = (z + length - 1) // length
    has_above = (2 * length - 2 - z) // length

    tail = rest - 1
    mixed = length == 4
    moves = n_prow == 4 and length <= 4
    giver = me_r == 2

    def by_class(at, act):
        if mixed:
            outer = ((at == 0) | (at == length - 1)) & jnp.logical_not(lead)
            pl.when(outer)(lambda: act(True))
            pl.when(jnp.logical_not(outer))(lambda: act(False))
        else:
            act(True)

    def columns_of(piece, kind):
        thick, given = kind if isinstance(kind, tuple) else (kind, False)
        start, size = cuts(gathered.shape[2], thick)[piece]
        return (start + LANES, size - LANES) if given and piece == tail else (start, size)

    def send(source, columns, send_sem, recv_sem, target):
        part = gathered.at[source, :, pl.ds(*columns)]
        pltpu.make_async_remote_copy(
            src_ref=part, dst_ref=part, send_sem=send_sem, recv_sem=recv_sem,
            device_id=(me_r, target), device_id_type=MESH,
        ).start()

    def arrival(columns, send_sem, recv_sem):
        count, size = box(columns, gathered.shape)
        part = gathered.at[pl.ds(0, count), :, pl.ds(0, size)]
        return pltpu.make_async_remote_copy(
            src_ref=part, dst_ref=part, send_sem=send_sem, recv_sem=recv_sem,
            device_id=(me_r, z * 2 + other), device_id_type=MESH,
        )

    def landed(columns, recv_sem):
        arrival(columns, sent.at[0], recv_sem).wait_recv()

    def neighbour(way):
        return me_c + 2 - 4 * way

    def slot(at, level):
        return at - (at > level).astype(jnp.int32)

    def line(way, at, piece, thick):
        send(
            at * 2 + x, columns_of(piece, thick), sent.at[way if piece < 2 else 2 + way], line_recv.at[slot(at, z + 1 - 2 * way), piece],
            neighbour(way),
        )

    def cross(at, piece, thick):
        send(at * 2 + x, columns_of(piece, thick), sent.at[4], cross_recv.at[piece], z * 2 + other)

    def line_rest(way, at, side, thick):
        send(at * 2 + side, columns_of(rest, thick), sent.at[2 + way], rest_recv.at[at], neighbour(way))

    def classed(at, piece, act):
        if piece == tail and moves:
            pl.when(giver)(lambda: by_class(at, lambda thick: act((thick, True))))
            pl.when(jnp.logical_not(giver))(lambda: by_class(at, act))
        elif piece >= tail:
            by_class(at, act)
        else:
            act(True)

    def both_ways(act):
        pl.when(z < length - 1)(lambda: act(0))
        pl.when(z > 0)(lambda: act(1))

    moved = pl.ds(pieces[tail][0], LANES)

    def guest_copy(source, target, recv_sem, row, column):
        return pltpu.make_async_remote_copy(
            src_ref=source, dst_ref=target, send_sem=guest_sem.at[4], recv_sem=recv_sem,
            device_id=(row, column), device_id_type=MESH,
        )

    def guest_total(count, recv_sem):
        rows_of, size = box(count * LANES, gathered.shape)
        part = gathered.at[pl.ds(0, rows_of), :, pl.ds(0, size)]
        return guest_copy(part, part, recv_sem, me_r, z * 2 + other)

    def only(who):
        return lambda act: pl.when(who)(act) if moves else None

    def guest_give():
        @only(giver)
        def _():
            guest_copy(gathered.at[me_c, :, moved], guest.at[me_c], guest_sem.at[0], 0, me_c).start()

    def guest_cross(source):
        part = guest.at[source]
        guest_copy(part, part, guest_sem.at[2], me_r, z * 2 + other).start()

    def guest_home(source):
        guest_copy(guest.at[source], gathered.at[source, :, moved], guest_sem.at[3], 2, me_c).start()

    def tell(n):
        @only(lead)
        def _():
            both_ways(lambda way: pl.semaphore_signal(
                ready.at[n], inc=1, device_id=(0, neighbour(way)), device_id_type=MESH
            ))

    def told(n):
        @only(lead)
        def _():
            pl.semaphore_wait(ready.at[n], has_below + has_above)

    def guest_own():
        told(1)

        @only(lead)
        def _():
            guest_total(1, guest_sem.at[0]).wait_recv()
            part = guest.at[me_c]
            for step in range(1, length):
                guest_copy(part, part, guest_sem.at[1], me_r, (z + step) % length * 2 + x).start()
            guest_cross(me_c)

    def guest_line():
        @only(lead)
        def _():
            guest_total(length - 1, guest_sem.at[1]).wait_recv()
            for step in range(1, length):
                guest_cross((z + step) % length * 2 + x)
            for step in range(1, length):
                guest_home((z + step) % length * 2 + x)

    def guest_other():
        @only(lead)
        def _():
            guest_total(length, guest_sem.at[2]).wait_recv()
            for at in range(length):
                guest_home(at * 2 + other)

    def guest_last():
        @only(giver)
        def _():
            guest_total(2 * length - 1, guest_sem.at[3]).wait_recv()

    def guest_drain():
        @only(giver)
        def _():
            guest_total(1, guest_sem.at[3]).wait_send()

        @only(lead)
        def _():
            guest_total(4 * length - 2, guest_sem.at[3]).wait_send()

    def first_sends():
        guest_give()
        for piece in bulk:
            def own(thick):
                both_ways(lambda way: line(way, z, piece, thick))
                cross(z, piece, thick)
            needed(piece, lambda: classed(z, piece, own))
            if piece == 2:
                by_class(z, lambda thick: send(
                    me_c, columns_of(rest, thick), sent.at[5], rest_recv.at[z], z * 2 + other
                ))
        own_rest(0, x)()

    def rest_ways(distance, act):
        if distance < length - 1:
            pl.when(z == distance)(lambda: act(0))
            pl.when(z == length - 1 - distance)(lambda: act(1))

    def own_rest(distance, side):
        def act(way):
            by_class(z, lambda thick: line_rest(way, z, side, thick))
        return lambda: rest_ways(distance, act)

    def other_rest():
        by_class(z, lambda thick: landed(columns_of(rest, thick)[1], rest_recv.at[z]))

    def both_rests(at, act=None):
        def classed_act(thick):
            landed(2 * columns_of(rest, thick)[1], rest_recv.at[at])
            if act is not None:
                for side in (0, 1):
                    act(side, thick)
        by_class(at, classed_act)

    def pass_rest(distance, reach):
        def onward(way):
            at = z + (2 * way - 1) * reach
            both_rests(at, lambda side, thick: line_rest(way, at, side, thick))
        return lambda: rest_ways(distance, onward)

    def relay(distance, piece):
        def both():
            for way, at, reached, onward in (
                (0, z - distance, z >= distance, z < length - 1),
                (1, z + distance, z < length - distance, z > 0),
            ):
                def pass_on(thick):
                    landed(columns_of(piece, thick)[1], line_recv.at[slot(at, z), piece])
                    pl.when(onward)(lambda: line(way, at, piece, thick))
                    cross(at, piece, thick)

                pl.when(reached)(lambda: classed(at, piece, pass_on))
        return lambda: needed(piece, both)

    def last_rests(distance):
        for way, at, reached in (
            (0, z - distance, (z >= distance) & (z == length - 1)),
            (1, z + distance, (z < length - distance) & (z == 0)),
        ):
            pl.when(reached)(lambda: both_rests(at))

    def lanes_of(pieces_of, levels, kind):
        leading, given = kind
        total = 0
        for at in levels:
            thick = not mixed or (not leading and at in (0, length - 1))
            for piece in pieces_of:
                start, size = columns_of(piece, (thick, given))
                total += 0 if leading and start + size <= block else size
        return total

    def for_kinds(act):
        pl.when(lead)(lambda: act((True, False)))
        if moves:
            pl.when(giver)(lambda: act((False, True)))
            pl.when(jnp.logical_not(lead | giver))(lambda: act((False, False)))
        else:
            pl.when(jnp.logical_not(lead))(lambda: act((False, False)))

    def crossed(piece):
        if piece == tail:
            for_kinds(lambda kind: landed(lanes_of([tail], range(length), kind), cross_recv.at[tail]))
        else:
            needed(piece, lambda: landed(length * pieces[piece][1], cross_recv.at[piece]))

    def drain():
        def gone(sem, columns):
            arrival(columns, sent.at[sem], rest_recv.at[0]).wait_send()

        def act(kind):
            for at in range(length):
                def here():
                    if at < length - 1:
                        gone(0, lanes_of(range(2), range(at + 1), kind))
                        gone(2, lanes_of([*range(2, rest), rest, rest], range(at + 1), kind))
                    if at > 0:
                        gone(1, lanes_of(range(2), range(at, length), kind))
                        gone(3, lanes_of([*range(2, rest), rest, rest], range(at, length), kind))
                    gone(5, lanes_of([rest], [at], kind))
                pl.when(z == at)(here)
            gone(4, lanes_of(bulk, range(length), kind))

        for_kinds(act)
        guest_drain()

    state = {}
    ii = iota((block, block), 0)
    jj = iota((block, block), 1)

    def column(row):
        return jnp.sum(jnp.where(ii == jj, row, 0.0), axis=1, keepdims=True)

    def bookkeeping():
        pivots_copy.wait()
        pivot_row = pivots_ref[...].astype(F32)
        pivot_col = column(pivot_row)
        chosen = jnp.max(jnp.where(pivot_col == jj.astype(F32), 1.0, 0.0), axis=0, keepdims=True)
        free = 1.0 - chosen
        far = jnp.where(pivot_row >= block, 1.0, 0.0)
        which = iota((16, block), 0)
        both = jnp.where(which == 0, free, jnp.where(which == 1, far, 0.0))
        ranks = dot(both.astype(BF16), jnp.where(ii < jj, 1.0, 0.0).astype(BF16))
        far_rank = column(ranks[1:2])
        match = (free > 0.5) & (ranks[0:1] == far_rank)
        source = jnp.sum(jnp.where(match, jj.astype(F32), 0.0), axis=1, keepdims=True)
        state.update(pivot_row=pivot_row, pivot_col=pivot_col, source=source)

    def pick():
        pivot_col, source = state["pivot_col"], state["source"]
        first = (me_r * rows).astype(F32)
        mine = (pivot_col >= first) & (pivot_col < first + rows)
        holds = lead.astype(F32)
        index = jnp.where(mine, pivot_col - first, source * holds - (1.0 - holds))
        slab_copy.wait()
        total = jnp.zeros((block, width), F32)
        for start in range(0, rows, block):
            hot = jnp.where((jj + start).astype(F32) == index, 1.0, 0.0).astype(BF16)
            total = total + dot(hot, slab_ref[start:start + block, :])
        picked[...] = total.astype(BF16)

    def core_copy():
        return pltpu.make_async_remote_copy(
            src_ref=picked, dst_ref=picked_in, send_sem=core_sem.at[0], recv_sem=core_sem.at[1],
            device_id=(peer, me_c), device_id_type=MESH,
        )

    def own_homes():
        homes[:, width:] = jnp.ones((block, LANES), BF16)

        @pl.when(me_r == 0)
        def _():
            hot = jnp.where(jj.astype(F32) == state["source"], 1.0, 0.0).astype(BF16)
            homes[:, :width] = dot(hot, slab_ref[:block, :]).astype(BF16)

    half = block // 2

    def chip_copy(step):
        rows_of = pl.ds(pl.multiple_of(core * half, half), half)
        to = ((chip + step) % chips) * 2 + core
        return pltpu.make_async_remote_copy(
            src_ref=merged.at[0, rows_of], dst_ref=merged.at[step, rows_of],
            send_sem=chip_send.at[step - 1], recv_sem=chip_recv.at[step - 1],
            device_id=(to, me_c), device_id_type=MESH,
        )

    def relay_copy(step):
        part = merged.at[step, pl.ds(pl.multiple_of(core * half, half), half)]
        return pltpu.make_async_remote_copy(
            src_ref=part, dst_ref=part, send_sem=relay_send.at[step - 1], recv_sem=relay_recv.at[step - 1],
            device_id=(peer, me_c), device_id_type=MESH,
        )

    def merge():
        core_copy().wait()
        pivot_col = state["pivot_col"]
        holds = (chip == 0).astype(F32)
        second = jnp.where((pivot_col >= rows) & (pivot_col < 2 * rows), holds, 0.0)
        mine, theirs = picked[...].astype(F32), picked_in[...].astype(F32)
        even = (core == 0).astype(F32)
        keep_mine = 1.0 - even * second
        keep_theirs = 1.0 - (1.0 - even) * second
        merged[0] = (mine * keep_mine + theirs * keep_theirs).astype(BF16)
        for step in range(1, chips):
            chip_copy(step).start()

    def relay_chips():
        for step in range(1, chips):
            chip_copy(step).wait()
            relay_copy(step).start()

    def assemble():
        for step in range(1, chips):
            relay_copy(step).wait()
        pivot_col = state["pivot_col"]
        top = jnp.zeros((block, width), F32)
        for step in range(chips):
            low = (((chip + chips - step) % chips) * 2 * rows).astype(F32)
            here = (pivot_col >= low) & (pivot_col < low + 2 * rows)
            top = top + jnp.where(here, merged[step].astype(F32), 0.0)
        state["top"] = top.astype(BF16)

        @pl.when(me_r == 1)
        def _():
            homes[:, :width] = picked_in[...]

        for step in range(1, chips):
            @pl.when((chip > 0) & (chip == step))
            def _():
                homes[:, :width] = merged[step]

    def interchange(start):
        def act():
            row = iota((block, block), 0) + (me_r * rows + start)
            pivot_row = state["pivot_row"]
            hot = jnp.where((row.astype(F32) == pivot_row) & (pivot_row >= block), 1.0, 0.0)
            both = dot(hot.astype(BF16), homes[...])
            taken = both[:, width:] > 0.5
            for lane in range(0, width, LANES):
                kept = slab_ref[start:start + block, lane:lane + LANES].astype(F32)
                new = jnp.where(taken, both[:, lane:lane + LANES], kept)
                pivoted[start:start + block, lane:lane + LANES] = new.astype(BF16)
        return act

    base = min(block, 256)
    small = min(base, 16)
    bi = iota((base, base), 0)
    bj = iota((base, base), 1)
    groups = block // base

    def diagonal(g):
        part = l_top_ref[g * base:(g + 1) * base, g * base:(g + 1) * base].astype(F32)
        return jnp.where(bi > bj, part, 0.0)

    def start_inverse():
        l_top_copy.wait()
        state["x"], state["power"] = [], []
        for g in range(groups):
            near = jnp.where(bi // small == bj // small, diagonal(g), 0.0)
            state["x"].append(jnp.where(bi == bj, 1.0, 0.0) - near)
            exact = near.astype(BF16)
            state["power"].append(dot(exact, exact))

    def power_step():
        for g in range(groups):
            x, power = state["x"][g], state["power"][g]
            state["x"][g] = x + dot_split(x, power)
            state["power"][g] = dot_split(power, power)

    def last_power():
        for g in range(groups):
            x, power = state["x"][g], state["power"][g]
            state["x"][g] = x + dot_split(x, power)

    def double(size):
        def act():
            for g in range(groups):
                link = jnp.where(
                    (bi // (2 * size) == bj // (2 * size)) & (bi // size != bj // size), diagonal(g), 0.0
                )
                inv = state["x"][g]
                state["x"][g] = inv - dot_split(inv, dot_exact_left(link.astype(BF16), inv))
        return act

    def join():
        for g in range(groups):
            high[g * base:(g + 1) * base, :] = jnp.zeros((base, block), F32)
            high[g * base:(g + 1) * base, g * base:(g + 1) * base] = state["x"][g]

    def join_double(size):
        def act():
            for at in range(0, block, 2 * size):
                a = high[at:at + size, at:at + size]
                b = high[at + size:at + 2 * size, at + size:at + 2 * size]
                c = l_top_ref[at + size:at + 2 * size, at:at + size]
                high[at + size:at + 2 * size, at:at + size] = -dot_split(b, dot_exact_left(c, a))
        return act

    def split():
        inverse_hi[...], inverse_lo[...] = halves(high[...])

    def solve():
        top = state["top"]
        u_ref[...] = (dot(inverse_hi[...], top) + dot(inverse_lo[...], top)).astype(BF16)

    inverse = [start_inverse]
    size = 4
    while size < small:
        inverse.append(power_step)
        size *= 2
    if small > 2:
        inverse.append(last_power)
    size = small
    while size < base:
        inverse.append(double(size))
        size *= 2
    inverse.append(join)
    while size < block:
        inverse.append(join_double(size))
        size *= 2
    inverse.append(split)

    def update(piece):
        start, size = pieces[piece]

        def act():
            panel = gathered[:, :, start:start + size].reshape(block, size).astype(BF16)
            out_ref[start:start + size, :] = trailing(panel, u_ref[...], pivoted[start:start + size, :])

        needed(piece, act)
        if start < block:
            @pl.when(lead)
            def _():
                end = min(block, start + size)
                out_ref[start:end, :] = u_ref[start:end, :]

    pl.semaphore_wait(barrier, 1 + chips + has_below + has_above)
    panel_copy.wait()
    first_sends()
    tell(0)
    bookkeeping()
    pick()
    core_copy().start()
    told(0)
    tell(1)

    own_homes()

    def relays(distance):
        return [relay(distance, piece) for piece in bulk] if distance < length else []

    changes = [interchange(start) for start in range(0, rows, block)]
    plan = inverse[:3] + [merge, guest_own] + weave(relays(1), inverse[3:6])
    plan += [other_rest, own_rest(0, other), own_rest(1, x), own_rest(1, other)] + inverse[6:8]
    second = relays(2)
    half_way = len(second) // 2
    plan += weave(second[:half_way], inverse[8:10]) + [guest_line, pass_rest(1, 1)]
    plan += weave(second[half_way:], [relay_chips] + inverse[10:])
    plan += [own_rest(2, x), own_rest(2, other), pass_rest(2, 1), assemble, solve]
    plan += weave(relays(3), changes[:3] + [pass_rest(2, 2)]) + changes[3:] + [guest_other]
    for distance in range(3, length):
        plan += relays(distance) if distance > 3 else []
        plan += [own_rest(distance, x), own_rest(distance, other)]
        plan += [pass_rest(distance, reach) for reach in range(1, distance + 1)]
    for act in plan:
        act()

    def near_levels():
        for distance in range(1, length - 1):
            last_rests(distance)
        start, size = columns_of(rest, False)
        total = pivoted[start:start + size, :].astype(F32)
        last = last_level(length)
        for step in range(1, length):
            total = total - level_of(gathered, u_ref, (last + step) % length, (start, size))
        partial[...] = total

    for piece in bulk:
        if piece == 0:
            pl.when(jnp.logical_not(lead))(near_levels)
        if piece == tail - 1:
            pl.when(lead)(near_levels)
        crossed(piece)
        if piece < tail:
            update(piece)
    last_rests(length - 1)
    guest_last()

    drain()


def finish(done_ref, gathered, u_ref, partial, pivoted, out_hbm, result, sem):
    block = u_ref.shape[0]
    edge = cuts(gathered.shape[2])[-2][0]
    start, size = cuts(gathered.shape[2], False)[-1]

    def store(source, start, size, n):
        copy = pltpu.make_async_copy(source, out_hbm.at[pl.ds(start, size)], sem.at[n])
        copy.start()
        return copy

    copies = [store(done_ref.at[pl.ds(0, edge)], 0, edge, 0)]
    last = last_level(gathered.shape[0] // 2)
    result[start - edge:, :] = (partial[...] - level_of(gathered, u_ref, last, (start, size))).astype(BF16)
    copies.append(store(result.at[pl.ds(start - edge, size)], start, size, 1))
    panel = gathered[:, :, edge:start].reshape(block, start - edge).astype(BF16)
    result[:start - edge, :] = trailing(panel, u_ref[...], pivoted[edge:start, :])
    copies.append(store(result.at[pl.ds(0, start - edge)], edge, start - edge, 2))
    for copy in copies:
        copy.wait()


def per_device(n_prow, n_pcol, slab, pivots, l_top, l_panel_t):
    rows, width = slab.shape
    block = pivots.shape[0]
    depth = l_panel_t.shape[0]
    kind = BF16 if depth % 16 == 0 else F32
    panel = l_panel_t.astype(kind)
    chips = n_prow // 2
    n_pieces = len(cuts(rows))
    vmem = pl.BlockSpec(memory_space=pltpu.VMEM)
    anywhere = pl.BlockSpec(memory_space=pltpu.HBM)
    dma = pltpu.SemaphoreType.DMA
    kept = [
        pltpu.VMEM((rows, width), BF16),
        pltpu.VMEM((n_pcol, depth, rows), kind),
        pltpu.VMEM((block, width), BF16),
        pltpu.VMEM((cuts(rows, False)[-1][1], width), F32),
        pltpu.VMEM((rows, width), BF16),
    ]
    done, gathered, u, partial, pivoted = pl.pallas_call(
        functools.partial(kernel, n_prow, n_pcol),
        out_shape=kept,
        in_specs=[anywhere] * 4,
        out_specs=[vmem] * 5,
        scratch_shapes=[
            pltpu.VMEM((rows, width), BF16),
            pltpu.VMEM((1, block), jnp.int32),
            pltpu.VMEM((block, block), BF16),
            pltpu.VMEM((block, width), BF16),
            pltpu.VMEM((block, width), BF16),
            pltpu.VMEM((chips, block, width), BF16),
            pltpu.VMEM((block, width + LANES), BF16),
            pltpu.VMEM((block, block), BF16),
            pltpu.VMEM((block, block), BF16),
            pltpu.VMEM((block, block), F32),
            pltpu.VMEM((n_pcol, depth, LANES), kind),
            dma((4,)),
            dma((n_pcol // 2 - 1, n_pieces - 1)),
            dma((n_pieces - 1,)),
            dma((n_pcol // 2,)),
            dma((6,)),
            dma((5,)),
            pltpu.SemaphoreType.REGULAR((2,)),
            dma((2,)),
            dma((chips - 1,)),
            dma((chips - 1,)),
            dma((chips - 1,)),
            dma((chips - 1,)),
        ],
        compiler_params=pltpu.CompilerParams(collective_id=0, has_side_effects=True, vmem_limit_bytes=LIMIT),
    )(slab, pivots.reshape(1, block), l_top, panel)
    return pl.pallas_call(
        finish,
        out_shape=pltpu.HBM((rows, width), BF16),
        in_specs=[vmem] * 5,
        out_specs=anywhere,
        scratch_shapes=[pltpu.VMEM((rows - cuts(rows)[-2][0], width), BF16), dma((3,))],
        compiler_params=pltpu.CompilerParams(vmem_limit_bytes=16 * 2**20),
    )(done, gathered, u, partial, pivoted)


def solution(mesh):
    return jax.shard_map(
        functools.partial(per_device, mesh.shape["prow"], mesh.shape["pcol"]),
        mesh=mesh,
        in_specs=(P("prow", "pcol"), P(), P(), P("pcol", "prow")),
        out_specs=P("prow", "pcol"),
        check_vma=False,
    )
```
